32 devices in a mesh: dom: 8 (over y, x, core), rep: 4 (over z).
Axes of the slice: x: 2, y: 2, z: 4, core: 2. Of those that a mesh axis runs over, the one named last changes fastest.
Arguments:
- right_sides: float32 [4, 48, 16, 384], P(None, 'dom', 'rep'), may hold values from -6 to 6
- diag_inverse: bfloat16 [4, 48, 384, 384], P(None, 'dom'), may hold values from -0.3125 to 0.3125
- panel_mats: bfloat16 [3, 512, 384, 384], P(None, ('dom', 'rep')), may hold values from -0.08984375 to 0.08984375
- panel_src: int32 [3, 512], P(None, ('dom', 'rep')), may hold values from 0 to 17, as said below
- panel_dst: int32 [3, 512], P(None, ('dom', 'rep')), may hold values from -1 to 47, as said below
Outputs:
- solution: float32 [4, 48, 16, 384], P(None, 'dom', 'rep')
The draws below stay inside these ranges and needn't reach their ends.
Inputs may be any that keep to these rules, and one draw needn't show every extreme that they name: `panel_src`: an entry of row l is below (l + 1) * 6, so the source tile lies in a level at most l; most of the entries lie in level l itself. A live entry of a list owned by dom index o names a tile of dom index (o + j) mod 8 with -2 <= j <= 2 or j = 4. Among the 16 entries of one device's list for one row, at most 3 live entries have the same destination dom index (panel_dst // 6), and in every list some dom index has exactly 3; lists of low dom indices tend to hold more live entries than those of high ones.
All inputs are finite; a program needn't handle non-finite values.
Results may differ from the reference program's by a relative error of at most 0.012.
Values may be sent and summed in bfloat16 or wider, within the bound.
A program may use at most 128 MiB of HBM per device.

```python
import jax
import jax.numpy as jnp
from jax import lax

CELLS = 128
NRHS = 16
TPL = 6
LEVELS = 4
HALF = 2
PPR = 16
TILES = 48
PANELS = 512
N_DOM = 8
N_REP = 4


def draw_panel_src(key, part):
    level_rows = LEVELS - 1
    entry_count = N_DOM * N_REP * PPR
    key_any, key_recent, key_choose = jax.random.split(jax.random.fold_in(key, 11), 3)
    row_index = jnp.arange(level_rows, dtype=jnp.int32)[:, None]
    anywhere = jax.random.randint(key_any, (level_rows, entry_count), 0, (row_index + 1) * TPL)
    recent = row_index * TPL + jax.random.randint(key_recent, (level_rows, entry_count), 0, TPL)
    chooser = jax.random.randint(key_choose, (level_rows, entry_count), 0, 2)
    return jnp.where(chooser == 0, recent, anywhere).astype(jnp.int32)


def draw_panel_dst(key, part):
    level_rows = LEVELS - 1
    block_count = N_DOM * N_REP
    hood = 2 * HALF + 2
    subkeys = jax.random.split(jax.random.fold_in(key, 23), 4)
    position = jnp.arange(PPR, dtype=jnp.int32)[None, None, :]
    owner = (jnp.arange(block_count, dtype=jnp.int32) // N_REP)[None, :, None]
    turn = jax.random.randint(subkeys[0], (level_rows, block_count, 1), 0, hood)
    klass = (position % hood + turn) % hood
    reach = jnp.where(klass == hood - 1, N_DOM // 2, klass - HALF)
    target = (owner + reach) % N_DOM
    dropper = jax.random.randint(subkeys[1], (level_rows, block_count, PPR), 0, 2 * N_DOM)
    padded = (position % hood != 0) & (dropper < owner + 1)
    column_slot = jax.random.randint(subkeys[2], (level_rows, block_count, PPR), 0, TPL)
    entries = jnp.where(padded, -1, target * TPL + column_slot)
    rotation = jax.random.randint(subkeys[3], (level_rows, block_count, 1), 0, PPR)
    reorder = (position + rotation) % PPR
    entries = jnp.take_along_axis(entries, reorder, axis=2)
    return entries.reshape(level_rows, block_count * PPR).astype(jnp.int32)


def block_levels(stream_key, extent, cuts, least, largest):
    gain, own = 1.0, jax.random.fold_in(stream_key, 6)
    for dim, blocks in cuts:
        heights = jnp.exp(jax.random.uniform(jax.random.fold_in(own, dim), (blocks,), jnp.float32, least / len(cuts), largest / len(cuts)))
        gain = gain * jnp.repeat(heights, extent[dim] // blocks).reshape([-1 if axis == dim else 1 for axis in range(len(extent))])
    return gain


def gaussian(key, extent, spread, limit, cuts=(), held_as=jnp.bfloat16):
    values = jax.random.normal(key, extent, jnp.float32) * spread
    if len(cuts) > 0:
        values = block_levels(key, extent, cuts, -0.22, 0.18) * values
    return jnp.clip(values, min=-limit, max=limit).astype(held_as)


def setup_inputs(seed: int = 0) -> dict:
    key_list = jax.random.split(jax.random.key(seed), 6)
    right_sides = gaussian(key_list[0], (LEVELS, TILES, NRHS, 3 * CELLS), 1.0, 6.0, ((1, 8), (2, 4)), jnp.float32)
    diag_inverse = gaussian(key_list[1], (LEVELS, TILES, 3 * CELLS, 3 * CELLS), (3 * CELLS) ** -0.5, 0.3125, ((1, 8),))
    panel_mats = gaussian(key_list[2], (LEVELS - 1, PANELS, 3 * CELLS, 3 * CELLS), 0.015, 0.08984375, ((1, 32),))
    panel_src = draw_panel_src(jax.random.fold_in(key_list[5], 71), 0)
    panel_dst = draw_panel_dst(jax.random.fold_in(key_list[5], 71), 0)
    return {"right_sides": right_sides, "diag_inverse": diag_inverse, "panel_mats": panel_mats, "panel_src": panel_src, "panel_dst": panel_dst}


def reference(right_sides, diag_inverse, panel_mats, panel_src, panel_dst):
    highest = lax.Precision.HIGHEST
    tile_total = N_DOM * TPL
    owner_dom = jnp.arange(N_DOM * N_REP * PPR, dtype=jnp.int32) // (N_REP * PPR)
    solved_all = []
    for level_index in range(LEVELS):
        residual = right_sides[level_index]
        if level_index > 0:
            history = jnp.stack([entry.astype(jnp.bfloat16) for entry in solved_all])
            source_ids = panel_src[level_index - 1]
            source_level = (source_ids // TPL).astype(jnp.int32)
            source_pos = (owner_dom * TPL + source_ids % TPL).astype(jnp.int32)
            sources = history[source_level, source_pos]
            contribution = jnp.einsum('qcx,qxy->qcy', sources.astype(jnp.float32), panel_mats[level_index - 1].astype(jnp.float32), precision=highest)
            onehot = (panel_dst[level_index - 1][:, None] == jnp.arange(tile_total, dtype=jnp.int32)[None, :]).astype(jnp.float32)
            incoming = jnp.einsum('qt,qcy->tcy', onehot, contribution, precision=highest)
            residual = residual - incoming
        rounded = lax.optimization_barrier(residual.astype(jnp.bfloat16))
        solved = jnp.einsum('tcx,txy->tcy', rounded.astype(jnp.float32), diag_inverse[level_index].astype(jnp.float32), precision=highest)
        solved_all.append(solved)
    return jnp.stack(solved_all)
```

```python
import functools

import jax
import jax.numpy as jnp
from jax import lax
from jax.experimental import pallas as pl
from jax.experimental.pallas import tpu as pltpu
from jax.sharding import PartitionSpec as P

HALF = 2
SLOTS = 3
HOOD = 2 * HALF + 2
MESH = pl.DeviceIdType.MESH
F32 = jnp.float32
BF16 = jnp.bfloat16


def iota(shape, dim):
    return lax.broadcasted_iota(jnp.int32, shape, dim).astype(F32)


def div(value, unit):
    return jnp.floor((value + 0.5) * (1.0 / unit))


def kernel(
    dims,
    src_hbm, dst_hbm, rs_hbm, diag_hbm, panel_hbm,
    out_ref,
    src_ref, dst_ref, rs_ref, small_sem,
    diag, panels_by_level, store, solved_ref, placed,
    slots_v, slots_s, slot_sem,
    val_send, val_recv, unpack, part_send, part_recv, id_send, id_recv,
    diag_sem, panel_sem, val_ssem, val_rsem, part_ssem, part_rsem, id_ssem, id_rsem,
):
    levels, tiles, cols, width, panels, dom_size, rep_size, chunk = dims
    far = dom_size // 2
    block = rep_size // 2 * cols
    tile_rows = tiles * block
    rows = SLOTS * block
    pairs = 2 * HOOD
    zero_tile = (levels - 1) * tiles
    me_d = lax.axis_index("dom")
    me_r = lax.axis_index("rep")
    my_half = lax.rem(me_r, 2)
    my_place = me_r // 2
    partner = me_r + 1 - 2 * my_half
    offsets = [o - HALF for o in range(HOOD - 1)] + [far]
    order = (HOOD - 1, 0, HOOD - 2, HALF, 1, HOOD - 3)

    def peer_dom(offset):
        return lax.rem(me_d + (offset + dom_size), dom_size)

    def peer_rep(step):
        return lax.rem(me_r + step, rep_size)

    peers = [(j, side) for j in order for side in (1, 0) if (offsets[j], side) != (0, 0)]
    others = [s for s in range(2, rep_size)] + [1]

    def load_diag(level):
        return pltpu.make_async_copy(diag_hbm.at[level], diag.at[level], diag_sem.at[level])

    def load_panel(level, part):
        span = pl.ds(part * chunk, chunk)
        return pltpu.make_async_copy(
            panel_hbm.at[level, span], panels_by_level[level].at[span], panel_sem.at[level, part]
        )

    def side_rep(side):
        return partner if side else me_r

    def side_half(side):
        return 1 - my_half if side else my_half

    def send_id(j, side):
        return pltpu.make_async_remote_copy(
            src_ref=id_send.at[j],
            dst_ref=id_recv.at[j, my_half],
            send_sem=id_ssem.at[j, side],
            recv_sem=id_rsem.at[j, my_half],
            device_id=(peer_dom(offsets[j]), side_rep(side)),
            device_id_type=MESH,
        )

    def await_id(j, side):
        pltpu.make_async_remote_copy(
            src_ref=id_send.at[j],
            dst_ref=id_recv.at[j, side_half(side)],
            send_sem=id_ssem.at[j, side],
            recv_sem=id_rsem.at[j, side_half(side)],
            device_id=(peer_dom(-offsets[j]), side_rep(side)),
            device_id_type=MESH,
        ).wait_recv()

    def send_val(level, j, side):
        return pltpu.make_async_remote_copy(
            src_ref=val_send.at[level, side_half(side), j],
            dst_ref=val_recv.at[level, j, my_half],
            send_sem=val_ssem.at[level, j, side],
            recv_sem=val_rsem.at[level, j, my_half],
            device_id=(peer_dom(offsets[j]), side_rep(side)),
            device_id_type=MESH,
        )

    def await_val(level, j, side):
        pltpu.make_async_remote_copy(
            src_ref=val_send.at[level, side_half(side), j],
            dst_ref=val_recv.at[level, j, side_half(side)],
            send_sem=val_ssem.at[level, j, side],
            recv_sem=val_rsem.at[level, j, side_half(side)],
            device_id=(peer_dom(-offsets[j]), side_rep(side)),
            device_id_type=MESH,
        ).wait_recv()

    def send_part(level, step):
        return pltpu.make_async_remote_copy(
            src_ref=part_send.at[level],
            dst_ref=part_recv.at[level, me_r],
            send_sem=part_ssem.at[level, step],
            recv_sem=part_rsem.at[level, me_r],
            device_id=(me_d, peer_rep(step)),
            device_id_type=MESH,
        )

    def await_part(level, step):
        slot = peer_rep(step)
        pltpu.make_async_remote_copy(
            src_ref=part_send.at[level],
            dst_ref=part_recv.at[level, slot],
            send_sem=part_ssem.at[level, step],
            recv_sem=part_rsem.at[level, slot],
            device_id=(me_d, slot),
            device_id_type=MESH,
        ).wait_recv()

    small = [
        pltpu.make_async_copy(hbm, ref, small_sem.at[i])
        for i, (hbm, ref) in enumerate(((rs_hbm, rs_ref), (dst_hbm, dst_ref), (src_hbm, src_ref)))
    ]
    for copy in small:
        copy.start()
    load_diag(0).start()
    for part in range(panels // chunk):
        load_panel(0, part).start()

    barrier = pltpu.get_barrier_semaphore()
    for j, side in peers:
        pl.semaphore_signal(
            barrier,
            inc=1,
            device_id=(peer_dom(offsets[j]), side_rep(side)),
            device_id_type=MESH,
        )
    for step in others:
        pl.semaphore_signal(
            barrier, inc=1, device_id=(me_d, peer_rep(step)), device_id_type=MESH
        )

    def place(level):
        row = lax.broadcasted_iota(jnp.int32, (block, width), 0) // cols
        for t in range(tiles):
            twice = jnp.concatenate([rs_ref[level, t]] * (rep_size // 2), axis=0)
            placed[level, t * block : (t + 1) * block] = jnp.where(row == my_place, twice, 0.0)

    def share(level, partial):
        rounded = partial.astype(BF16)
        part_send[level] = rounded
        return rounded

    def route():
        owner = me_d.astype(F32)
        row16 = iota((panels, panels), 0)
        col16 = iota((panels, panels), 1)
        lane = iota((1, 128), 1)
        id_level = div(lane, rows)
        id_rest = lane - rows * id_level
        id_slot = div(id_rest, block)
        id_col = id_rest - block * id_slot
        panel_col = iota((panels, 1), 0)
        wanted = [jnp.zeros((1, 128), F32) for _ in range(HOOD)]
        for l in range(levels - 1):
            drow = dst_ref[l : l + 1, :].astype(F32)
            srow = src_ref[l : l + 1, :].astype(F32)
            dcol = jnp.sum(jnp.where(row16 == col16, drow, 0.0), axis=1, keepdims=True)
            scol = jnp.sum(jnp.where(row16 == col16, srow, 0.0), axis=1, keepdims=True)
            trow = jnp.where(drow >= 0, div(drow, tiles), -1.0)
            tcol = jnp.where(dcol >= 0, div(dcol, tiles), -1.0)
            earlier = (tcol == trow) & (drow >= 0) & (col16 < row16)
            rank = jnp.sum(jnp.where(earlier, 1.0, 0.0), axis=1, keepdims=True)
            away = tcol - owner
            away = away + jnp.where(away < 0, float(dom_size), 0.0)
            near = away + HALF
            near = near - jnp.where(near >= dom_size, float(dom_size), 0.0)
            reach = jnp.where(away == far, float(HOOD - 1), near)
            reach = jnp.where(dcol >= 0, reach, -1.0)
            spot = jnp.where(dcol >= 0, reach * SLOTS + rank, -1.0)
            tile = dcol - tiles * tcol
            here = spot == lane
            which = jnp.sum(jnp.where(here, panel_col, 0.0), axis=0, keepdims=True)
            source = jnp.sum(jnp.where(here, scol - zero_tile, 0.0), axis=0, keepdims=True)
            slots_v[2 * l : 2 * l + 1, :] = which.astype(jnp.int32)
            slots_v[2 * l + 1 : 2 * l + 2, :] = (source + zero_tile).astype(jnp.int32)
            mine = (rank == id_slot) & (id_level == l)
            for j in range(HOOD):
                found = jnp.where(mine & (reach == j), tile + 1.0, 0.0)
                wanted[j] = wanted[j] + jnp.sum(found, axis=0, keepdims=True)
        for j in range(HOOD):
            row = jnp.where(wanted[j] > 0, (wanted[j] - 1.0) * block + id_col, -1.0)
            id_send[j] = row.astype(jnp.int32)
        id_recv[HALF, my_half] = id_send[HALF]

    def learn_ids():
        for j, side in peers:
            await_id(j, side)
        row_of = iota((pairs, 128), 0)
        ids = jnp.zeros((pairs, 128), F32)
        for j in range(HOOD):
            for h in range(2):
                ids = jnp.where(row_of == 2 * j + h, id_recv[j, h].astype(F32), ids)
        ids = ids.astype(BF16)
        span = pairs * rows
        lane = iota((1, span), 1)
        lane_sender = div(lane, rows)
        lane_in = lane - rows * lane_sender
        for l in range(levels - 1):
            take = jnp.where(iota((128, span), 0) == lane_in + l * rows, 1.0, 0.0)
            every = jnp.dot(ids, take.astype(BF16), preferred_element_type=F32)
            own = jnp.where(iota((pairs, span), 0) == lane_sender, every, 0.0)
            goal = jnp.sum(own, axis=0, keepdims=True)
            unpack[l] = jnp.where(iota((tile_rows, span), 0) == goal, 1.0, 0.0).astype(BF16)

    def emit(level):
        for t in range(tiles):
            mine = solved_ref[level, t, my_half]
            picked = mine[:cols]
            for q in range(1, rep_size // 2):
                picked = jnp.where(my_place == q, mine[q * cols : (q + 1) * cols], picked)
            out_ref[level, t] = picked

    small[0].wait()
    place(0)
    rounded = share(0, placed[0])
    pl.semaphore_wait(barrier, len(peers) + len(others))
    for step in others:
        send_part(0, step).start()
    part_recv[0, me_r] = rounded
    small[1].wait()
    small[2].wait()
    route()
    slot_copy = pltpu.make_async_copy(slots_v, slots_s, slot_sem)
    slot_copy.start()
    for j, side in peers:
        send_id(j, side).start()
    for level in range(1, levels):
        place(level)
    store[zero_tile] = jnp.zeros((2 * block, width), BF16)

    for level in range(levels):
        for step in others:
            await_part(level, step)
        halves = []
        for h in range(2):
            total = part_recv[level, h].astype(F32)
            for r in range(h + 2, rep_size, 2):
                total = total + part_recv[level, r].astype(F32)
            halves.append(total)
        load_diag(level).wait()
        for t in range(tiles):
            span = slice(t * block, (t + 1) * block)
            residual = jnp.concatenate([half[span] for half in halves], axis=0).astype(BF16)
            solved = jnp.dot(residual, diag[level, t], preferred_element_type=F32)
            if level + 1 < levels:
                store[level * tiles + t] = solved.astype(BF16)
            for h in range(2):
                solved_ref[level, t, h] = solved[h * block : (h + 1) * block]
        if level + 1 == levels:
            break
        if level == 0:
            slot_copy.wait()
        for part in range(panels // chunk):
            load_panel(level, part).wait()
        for j in order:
            for k in range(SLOTS):
                which = jnp.clip(slots_s[2 * level, j * SLOTS + k], 0, panels - 1)
                source = jnp.clip(slots_s[2 * level + 1, j * SLOTS + k], 0, zero_tile)
                product = jnp.dot(
                    store[source], panels_by_level[level][which], preferred_element_type=F32
                ).astype(BF16)
                for h in range(2):
                    val_send[level, h, j, k * block : (k + 1) * block] = product[
                        h * block : (h + 1) * block
                    ]
            for side in (1, 0):
                if (j, side) in peers:
                    send_val(level, j, side).start()
        val_recv[level, HALF, my_half] = val_send[level, my_half, HALF]
        load_diag(level + 1).start()
        if level + 2 < levels:
            for part in range(panels // chunk):
                load_panel(level + 1, part).start()
        if level == 0:
            learn_ids()
        emit(level)
        for j, side in peers:
            await_val(level, j, side)
        arrived = val_recv[level].reshape(pairs * rows, width)
        incoming = jnp.dot(unpack[level], arrived, preferred_element_type=F32)
        rounded = share(level + 1, placed[level + 1] - incoming)
        for step in others:
            send_part(level + 1, step).start()
        part_recv[level + 1, me_r] = rounded

    emit(levels - 1)
    for j, side in peers:
        send_id(j, side).wait_send()
        for level in range(levels - 1):
            send_val(level, j, side).wait_send()
    for step in others:
        for level in range(levels):
            send_part(level, step).wait_send()


def per_device(right_sides, diag_inverse, panel_mats, panel_src, panel_dst):
    levels, tiles, cols, width = right_sides.shape
    panels = panel_mats.shape[1]
    dom_size = lax.axis_size("dom")
    rep_size = lax.axis_size("rep")
    block = rep_size // 2 * cols
    tile_rows = tiles * block
    rows = SLOTS * block
    chunk = 4 if panels % 4 == 0 else 1
    assert rep_size % 2 == 0 and block % 8 == 0 and (levels - 1) * rows <= 128
    dims = (levels, tiles, cols, width, panels, dom_size, rep_size, chunk)
    vmem = pl.BlockSpec(memory_space=pltpu.VMEM)
    hbm = pl.BlockSpec(memory_space=pl.ANY)
    dma = pltpu.SemaphoreType.DMA
    i32 = jnp.int32
    return pl.pallas_call(
        functools.partial(kernel, dims),
        out_shape=jax.ShapeDtypeStruct(right_sides.shape, F32),
        in_specs=[hbm] * 5,
        out_specs=vmem,
        scratch_shapes=[
            pltpu.VMEM(panel_src.shape, i32),
            pltpu.VMEM(panel_dst.shape, i32),
            pltpu.VMEM(right_sides.shape, F32),
            dma((3,)),
            pltpu.VMEM(diag_inverse.shape, BF16),
            [pltpu.VMEM(panel_mats.shape[1:], BF16) for _ in range(levels - 1)],
            pltpu.VMEM(((levels - 1) * tiles + 1, 2 * block, width), BF16),
            pltpu.VMEM((levels, tiles, 2, block, width), F32),
            pltpu.VMEM((levels, tile_rows, width), F32),
            pltpu.VMEM((8, 128), i32),
            pltpu.SMEM((8, 128), i32),
            dma,
            pltpu.VMEM((levels - 1, 2, HOOD, rows, width), BF16),
            pltpu.VMEM((levels - 1, HOOD, 2, rows, width), BF16),
            pltpu.VMEM((levels - 1, tile_rows, 2 * HOOD * rows), BF16),
            pltpu.VMEM((levels, tile_rows, width), BF16),
            pltpu.VMEM((levels, rep_size, tile_rows, width), BF16),
            pltpu.VMEM((HOOD, 1, 128), i32),
            pltpu.VMEM((HOOD, 2, 1, 128), i32),
            dma((levels,)),
            dma((levels - 1, panels // chunk)),
            dma((levels - 1, HOOD, 2)),
            dma((levels - 1, HOOD, 2)),
            dma((levels, rep_size)),
            dma((levels, rep_size)),
            dma((HOOD, 2)),
            dma((HOOD, 2)),
        ],
        compiler_params=pltpu.CompilerParams(
            collective_id=0, has_side_effects=True, vmem_limit_bytes=67043328
        ),
    )(panel_src, panel_dst, right_sides, diag_inverse, panel_mats)


def solution(mesh):
    return jax.shard_map(
        per_device,
        mesh=mesh,
        in_specs=(
            P(None, "dom", "rep", None),
            P(None, "dom", None, None),
            P(None, ("dom", "rep"), None, None),
            P(None, ("dom", "rep")),
            P(None, ("dom", "rep")),
        ),
        out_specs=P(None, "dom", "rep", None),
        check_vma=False,
    )
```

```python
import functools

import jax
import jax.numpy as jnp
from jax import lax
from jax.experimental import pallas as pl
from jax.experimental.pallas import tpu as pltpu
from jax.sharding import PartitionSpec as P

HALF = 2
SLOTS = 3
HOOD = 2 * HALF + 2
MESH = pl.DeviceIdType.MESH
F32 = jnp.float32
BF16 = jnp.bfloat16


def iota(shape, dim):
    return lax.broadcasted_iota(jnp.int32, shape, dim).astype(F32)


def div(value, unit):
    return jnp.floor((value + 0.5) * (1.0 / unit))


def kernel(
    dims,
    src_hbm, dst_hbm, rs_hbm, diag_hbm, panel_hbm,
    out_ref,
    src_ref, dst_ref, rs_ref, small_sem,
    diag, panels_by_level, store, solved_ref, placed,
    slots_v, slots_s, slot_sem,
    val_send, val_recv, unpack, part_send, part_recv, id_send, id_recv,
    last_send, last_recv, last_unpack,
    diag_sem, panel_sem, val_ssem, val_rsem, part_ssem, part_rsem, id_ssem, id_rsem,
    last_ssem, last_rsem,
):
    levels, tiles, cols, width, panels, dom_size, rep_size, chunk = dims
    far = dom_size // 2
    block = rep_size // 2 * cols
    tile_rows = tiles * block
    rows = SLOTS * block
    pairs = 2 * HOOD
    senders = HOOD * rep_size
    half_rows = 2 * cols
    third = width // 3
    own_rows = tiles * cols
    last = levels - 2
    zero_tile = (levels - 1) * tiles
    me_d = lax.axis_index("dom")
    me_r = lax.axis_index("rep")
    my_half = lax.rem(me_r, 2)
    my_place = me_r // 2
    partner = me_r + 1 - 2 * my_half
    offsets = [o - HALF for o in range(HOOD - 1)] + [far]
    order = (HOOD - 1, 0, HOOD - 2, HALF, 1, HOOD - 3)

    def peer_dom(offset):
        return lax.rem(me_d + (offset + dom_size), dom_size)

    def peer_rep(step):
        return lax.rem(me_r + step, rep_size)

    peers = [(j, side) for j in order for side in (1, 0) if (offsets[j], side) != (0, 0)]
    others = [s for s in range(2, rep_size)] + [1]
    everyone = [(j, step) for j in order for step in others + [0] if (offsets[j], step) != (0, 0)]

    def load_diag(level):
        return pltpu.make_async_copy(diag_hbm.at[level], diag.at[level], diag_sem.at[level])

    def load_panel(level, part):
        span = pl.ds(part * chunk, chunk)
        return pltpu.make_async_copy(
            panel_hbm.at[level, span], panels_by_level[level].at[span], panel_sem.at[level, part]
        )

    def side_rep(side):
        return partner if side else me_r

    def side_half(side):
        return 1 - my_half if side else my_half

    def send_id(j, step):
        return pltpu.make_async_remote_copy(
            src_ref=id_send.at[j],
            dst_ref=id_recv.at[j, me_r],
            send_sem=id_ssem.at[j, step],
            recv_sem=id_rsem.at[j, me_r],
            device_id=(peer_dom(offsets[j]), peer_rep(step)),
            device_id_type=MESH,
        )

    def await_id(j, step):
        slot = peer_rep(step)
        pltpu.make_async_remote_copy(
            src_ref=id_send.at[j],
            dst_ref=id_recv.at[j, slot],
            send_sem=id_ssem.at[j, step],
            recv_sem=id_rsem.at[j, slot],
            device_id=(peer_dom(-offsets[j]), slot),
            device_id_type=MESH,
        ).wait_recv()

    def send_last(j, step):
        return pltpu.make_async_remote_copy(
            src_ref=last_send.at[j, peer_rep(step)],
            dst_ref=last_recv.at[j, me_r],
            send_sem=last_ssem.at[j, step],
            recv_sem=last_rsem.at[j, me_r],
            device_id=(peer_dom(offsets[j]), peer_rep(step)),
            device_id_type=MESH,
        )

    def await_last(j, step):
        slot = peer_rep(step)
        pltpu.make_async_remote_copy(
            src_ref=last_send.at[j, slot],
            dst_ref=last_recv.at[j, slot],
            send_sem=last_ssem.at[j, step],
            recv_sem=last_rsem.at[j, slot],
            device_id=(peer_dom(-offsets[j]), slot),
            device_id_type=MESH,
        ).wait_recv()

    def send_val(level, j, side):
        return pltpu.make_async_remote_copy(
            src_ref=val_send.at[level, side_half(side), j],
            dst_ref=val_recv.at[level, j, my_half],
            send_sem=val_ssem.at[level, j, side],
            recv_sem=val_rsem.at[level, j, my_half],
            device_id=(peer_dom(offsets[j]), side_rep(side)),
            device_id_type=MESH,
        )

    def await_val(level, j, side):
        pltpu.make_async_remote_copy(
            src_ref=val_send.at[level, side_half(side), j],
            dst_ref=val_recv.at[level, j, side_half(side)],
            send_sem=val_ssem.at[level, j, side],
            recv_sem=val_rsem.at[level, j, side_half(side)],
            device_id=(peer_dom(-offsets[j]), side_rep(side)),
            device_id_type=MESH,
        ).wait_recv()

    def part_span(level):
        return pl.ds(0, tile_rows if level else own_rows)

    def send_part(level, step):
        return pltpu.make_async_remote_copy(
            src_ref=part_send.at[level, part_span(level)],
            dst_ref=part_recv.at[level, me_r, part_span(level)],
            send_sem=part_ssem.at[level, step],
            recv_sem=part_rsem.at[level, me_r],
            device_id=(me_d, peer_rep(step)),
            device_id_type=MESH,
        )

    def await_part(level, step):
        slot = peer_rep(step)
        pltpu.make_async_remote_copy(
            src_ref=part_send.at[level, part_span(level)],
            dst_ref=part_recv.at[level, slot, part_span(level)],
            send_sem=part_ssem.at[level, step],
            recv_sem=part_rsem.at[level, slot],
            device_id=(me_d, slot),
            device_id_type=MESH,
        ).wait_recv()

    small = [
        pltpu.make_async_copy(hbm, ref, small_sem.at[i])
        for i, (hbm, ref) in enumerate(((rs_hbm, rs_ref), (dst_hbm, dst_ref), (src_hbm, src_ref)))
    ]
    for copy in small:
        copy.start()
    load_diag(0).start()
    for part in range(panels // chunk):
        load_panel(0, part).start()

    barrier = pltpu.get_barrier_semaphore()
    for j, step in everyone:
        pl.semaphore_signal(
            barrier,
            inc=1,
            device_id=(peer_dom(offsets[j]), peer_rep(step)),
            device_id_type=MESH,
        )

    def place(level):
        row = lax.broadcasted_iota(jnp.int32, (block, width), 0) // cols
        for t in range(tiles):
            twice = jnp.concatenate([rs_ref[level, t]] * (rep_size // 2), axis=0)
            placed[level, t * block : (t + 1) * block] = jnp.where(row == my_place, twice, 0.0)

    def share(level, partial):
        rounded = partial.astype(BF16)
        part_send[level, : rounded.shape[0]] = rounded
        for step in others:
            send_part(level, step).start()
        part_recv[level, me_r, : rounded.shape[0]] = rounded

    def route():
        owner = me_d.astype(F32)
        row16 = iota((panels, panels), 0)
        col16 = iota((panels, panels), 1)
        lane = iota((1, 128), 1)
        id_level = div(lane, rows)
        id_rest = lane - rows * id_level
        id_slot = div(id_rest, block)
        id_col = id_rest - block * id_slot
        panel_col = iota((panels, 1), 0)
        wanted = [jnp.zeros((1, 128), F32) for _ in range(HOOD)]
        for l in range(levels - 1):
            drow = dst_ref[l : l + 1, :].astype(F32)
            srow = src_ref[l : l + 1, :].astype(F32)
            dcol = jnp.sum(jnp.where(row16 == col16, drow, 0.0), axis=1, keepdims=True)
            scol = jnp.sum(jnp.where(row16 == col16, srow, 0.0), axis=1, keepdims=True)
            trow = jnp.where(drow >= 0, div(drow, tiles), -1.0)
            tcol = jnp.where(dcol >= 0, div(dcol, tiles), -1.0)
            earlier = (tcol == trow) & (drow >= 0) & (col16 < row16)
            rank = jnp.sum(jnp.where(earlier, 1.0, 0.0), axis=1, keepdims=True)
            away = tcol - owner
            away = away + jnp.where(away < 0, float(dom_size), 0.0)
            near = away + HALF
            near = near - jnp.where(near >= dom_size, float(dom_size), 0.0)
            reach = jnp.where(away == far, float(HOOD - 1), near)
            reach = jnp.where(dcol >= 0, reach, -1.0)
            spot = jnp.where(dcol >= 0, reach * SLOTS + rank, -1.0)
            tile = dcol - tiles * tcol
            here = spot == lane
            which = jnp.sum(jnp.where(here, panel_col, 0.0), axis=0, keepdims=True)
            source = jnp.sum(jnp.where(here, scol - zero_tile, 0.0), axis=0, keepdims=True)
            slots_v[2 * l : 2 * l + 1, :] = which.astype(jnp.int32)
            slots_v[2 * l + 1 : 2 * l + 2, :] = (source + zero_tile).astype(jnp.int32)
            if l == last:
                id_slot = div(id_rest, cols)
                id_col = id_rest - cols * id_slot
            mine = (rank == id_slot) & (id_level == l)
            for j in range(HOOD):
                spread = tile * (cols if l == last else block) + id_col + 1.0
                found = jnp.where(mine & (reach == j), spread, 0.0)
                wanted[j] = wanted[j] + jnp.sum(found, axis=0, keepdims=True)
        for j in range(HOOD):
            id_send[j] = (wanted[j] - 1.0).astype(jnp.int32)
        id_recv[HALF, me_r] = id_send[HALF]

    def learn_ids():
        for j, step in everyone:
            await_id(j, step)

        def lookup(ids, count, span, lane_in):
            lane_sender = div(iota((1, span), 1), span // count)
            take = jnp.where(iota((128, span), 0) == lane_in, 1.0, 0.0)
            every = jnp.dot(ids, take.astype(BF16), preferred_element_type=F32)
            own = jnp.where(iota((count, span), 0) == lane_sender, every, 0.0)
            return jnp.sum(own, axis=0, keepdims=True)

        near = jnp.zeros((pairs, 128), F32)
        full = jnp.zeros((senders, 128), F32)
        for j in range(HOOD):
            for side in range(2):
                row = id_recv[j, my_place * 2 + side].astype(F32)
                near = jnp.where(iota((pairs, 128), 0) == 2 * j + side, row, near)
            for r in range(rep_size):
                row = id_recv[j, r].astype(F32)
                full = jnp.where(iota((senders, 128), 0) == rep_size * j + r, row, full)
        span = pairs * rows
        lane = iota((1, span), 1)
        lane_in = lane - rows * div(lane, rows)
        for l in range(last):
            goal = lookup(near.astype(BF16), pairs, span, lane_in + l * rows)
            unpack[l] = jnp.where(iota((tile_rows, span), 0) == goal, 1.0, 0.0).astype(BF16)
        span = senders * half_rows
        lane = iota((1, span), 1)
        lane_in = lane - half_rows * div(lane, half_rows)
        low = lane_in < cols
        full = full.astype(BF16)
        first = lookup(full, senders, span, lane_in + last * rows)
        fold = lookup(full, senders, span, lane_in + last * rows + jnp.where(low, 2.0 * cols, 1.0 * cols))
        for i, goal in enumerate((first, jnp.where(low, fold, -1.0), jnp.where(low, -1.0, fold))):
            last_unpack[i] = jnp.where(iota((own_rows, span), 0) == goal, 1.0, 0.0).astype(BF16)

    def emit(level):
        for t in range(tiles):
            mine = solved_ref[level, t, my_half]
            picked = mine[:cols]
            for q in range(1, rep_size // 2):
                picked = jnp.where(my_place == q, mine[q * cols : (q + 1) * cols], picked)
            out_ref[level, t] = picked

    def own_sides(level):
        return jnp.concatenate([rs_ref[level, t] for t in range(tiles)], axis=0)

    small[0].wait()
    pl.semaphore_wait(barrier, len(everyone))
    share(0, own_sides(0))
    small[1].wait()
    small[2].wait()
    route()
    slot_copy = pltpu.make_async_copy(slots_v, slots_s, slot_sem)
    slot_copy.start()
    for j, step in everyone:
        send_id(j, step).start()
    for level in range(1, levels - 1):
        place(level)
    store[zero_tile] = jnp.zeros((2 * block, width), BF16)

    for level in range(levels - 1):
        for step in others:
            await_part(level, step)
        if level == 0:
            parts = [part_recv[0, r, :own_rows].astype(F32) for r in range(rep_size)]
            residuals = [
                jnp.concatenate(
                    [
                        parts[r][t * cols : (t + 1) * cols]
                        for h in range(2)
                        for r in range(h, rep_size, 2)
                    ],
                    axis=0,
                )
                for t in range(tiles)
            ]
        else:
            halves = []
            for h in range(2):
                total = part_recv[level, h].astype(F32)
                for r in range(h + 2, rep_size, 2):
                    total = total + part_recv[level, r].astype(F32)
                halves.append(total)
            residuals = [
                jnp.concatenate([half[t * block : (t + 1) * block] for half in halves], axis=0)
                for t in range(tiles)
            ]
        load_diag(level).wait()
        for t in range(tiles):
            residual = residuals[t].astype(BF16)
            solved = jnp.dot(residual, diag[level, t], preferred_element_type=F32)
            store[level * tiles + t] = solved.astype(BF16)
            for h in range(2):
                solved_ref[level, t, h] = solved[h * block : (h + 1) * block]
        if level == 0:
            slot_copy.wait()
        for part in range(panels // chunk):
            load_panel(level, part).wait()
        for j in order:
            products = []
            for k in range(SLOTS):
                which = jnp.clip(slots_s[2 * level, j * SLOTS + k], 0, panels - 1)
                source = jnp.clip(slots_s[2 * level + 1, j * SLOTS + k], 0, zero_tile)
                products.append(
                    jnp.dot(
                        store[source], panels_by_level[level][which], preferred_element_type=F32
                    )
                )
            if level < last:
                for k in range(SLOTS):
                    rounded = products[k].astype(BF16)
                    for h in range(2):
                        val_send[level, h, j, k * block : (k + 1) * block] = rounded[
                            h * block : (h + 1) * block
                        ]
                for side in (1, 0):
                    if (j, side) in peers:
                        send_val(level, j, side).start()
            else:
                for r in range(rep_size):
                    begin = r % 2 * block + r // 2 * cols
                    piece = [p[begin : begin + cols] for p in products]
                    last_send[j, r, :, :width] = jnp.concatenate(piece[:2], axis=0).astype(BF16)
                    tail = piece[2]
                    mixed = jnp.concatenate([tail[:, :third], tail[:, 2 * third :]], axis=0)
                    again = jnp.concatenate([tail[:, third : 2 * third]] * 2, axis=0)
                    last_send[j, r, :, width : width + third] = mixed.astype(BF16)
                    last_send[j, r, :, width + third :] = again.astype(BF16)
                for step in others + [0]:
                    if (j, step) in everyone:
                        send_last(j, step).start()
        if level < last:
            val_recv[level, HALF, my_half] = val_send[level, my_half, HALF]
        else:
            last_recv[HALF, me_r] = last_send[HALF, me_r]
        load_diag(level + 1).start()
        if level < last:
            for part in range(panels // chunk):
                load_panel(level + 1, part).start()
        if level == 0:
            learn_ids()
        emit(level)
        if level < last:
            for j, side in peers:
                await_val(level, j, side)
            arrived = val_recv[level].reshape(pairs * rows, width)
            incoming = jnp.dot(unpack[level], arrived, preferred_element_type=F32)
            share(level + 1, placed[level + 1] - incoming)

    for j, step in everyone:
        await_last(j, step)
    arrived = last_recv[...].reshape(senders * half_rows, width + 2 * third)
    folded = arrived[:, width:]
    whole = jnp.dot(last_unpack[0], arrived[:, :width], preferred_element_type=F32)
    low = jnp.dot(last_unpack[1], folded, preferred_element_type=F32)
    high = jnp.dot(last_unpack[2], folded[:, :third], preferred_element_type=F32)
    residual = own_sides(levels - 1) - (whole + jnp.concatenate([low, high], axis=1))
    residual = residual.astype(BF16)
    load_diag(levels - 1).wait()
    for t in range(tiles):
        solved = jnp.dot(residual, diag[levels - 1, t], preferred_element_type=F32)
        out_ref[levels - 1, t] = solved[t * cols : (t + 1) * cols]

    for j, step in everyone:
        send_id(j, step).wait_send()
        send_last(j, step).wait_send()
    for j, side in peers:
        for level in range(last):
            send_val(level, j, side).wait_send()
    for step in others:
        for level in range(levels - 1):
            send_part(level, step).wait_send()


def per_device(right_sides, diag_inverse, panel_mats, panel_src, panel_dst):
    levels, tiles, cols, width = right_sides.shape
    panels = panel_mats.shape[1]
    dom_size = lax.axis_size("dom")
    rep_size = lax.axis_size("rep")
    block = rep_size // 2 * cols
    tile_rows = tiles * block
    rows = SLOTS * block
    chunk = 4 if panels % 4 == 0 else 1
    assert rep_size % 2 == 0 and block % 8 == 0 and (levels - 1) * rows <= 128
    assert 2 * cols == 8 and width % 384 == 0 and levels > 2
    dims = (levels, tiles, cols, width, panels, dom_size, rep_size, chunk)
    vmem = pl.BlockSpec(memory_space=pltpu.VMEM)
    hbm = pl.BlockSpec(memory_space=pl.ANY)
    dma = pltpu.SemaphoreType.DMA
    i32 = jnp.int32
    return pl.pallas_call(
        functools.partial(kernel, dims),
        out_shape=jax.ShapeDtypeStruct(right_sides.shape, F32),
        in_specs=[hbm] * 5,
        out_specs=vmem,
        scratch_shapes=[
            pltpu.VMEM(panel_src.shape, i32),
            pltpu.VMEM(panel_dst.shape, i32),
            pltpu.VMEM(right_sides.shape, F32),
            dma((3,)),
            pltpu.VMEM(diag_inverse.shape, BF16),
            [pltpu.VMEM(panel_mats.shape[1:], BF16) for _ in range(levels - 1)],
            pltpu.VMEM(((levels - 1) * tiles + 1, 2 * block, width), BF16),
            pltpu.VMEM((levels - 1, tiles, 2, block, width), F32),
            pltpu.VMEM((levels - 1, tile_rows, width), F32),
            pltpu.VMEM((8, 128), i32),
            pltpu.SMEM((8, 128), i32),
            dma,
            pltpu.VMEM((levels - 2, 2, HOOD, rows, width), BF16),
            pltpu.VMEM((levels - 2, HOOD, 2, rows, width), BF16),
            pltpu.VMEM((levels - 2, tile_rows, 2 * HOOD * rows), BF16),
            pltpu.VMEM((levels - 1, tile_rows, width), BF16),
            pltpu.VMEM((levels - 1, rep_size, tile_rows, width), BF16),
            pltpu.VMEM((HOOD, 1, 128), i32),
            pltpu.VMEM((HOOD, rep_size, 1, 128), i32),
            pltpu.VMEM((HOOD, rep_size, 2 * cols, width + width // 3 * 2), BF16),
            pltpu.VMEM((HOOD, rep_size, 2 * cols, width + width // 3 * 2), BF16),
            pltpu.VMEM((3, tiles * cols, HOOD * rep_size * 2 * cols), BF16),
            dma((levels,)),
            dma((levels - 1, panels // chunk)),
            dma((levels - 2, HOOD, 2)),
            dma((levels - 2, HOOD, 2)),
            dma((levels - 1, rep_size)),
            dma((levels - 1, rep_size)),
            dma((HOOD, rep_size)),
            dma((HOOD, rep_size)),
            dma((HOOD, rep_size)),
            dma((HOOD, rep_size)),
        ],
        compiler_params=pltpu.CompilerParams(
            collective_id=0, has_side_effects=True, vmem_limit_bytes=67043328
        ),
    )(panel_src, panel_dst, right_sides, diag_inverse, panel_mats)


def solution(mesh):
    return jax.shard_map(
        per_device,
        mesh=mesh,
        in_specs=(
            P(None, "dom", "rep", None),
            P(None, "dom", None, None),
            P(None, ("dom", "rep"), None, None),
            P(None, ("dom", "rep")),
            P(None, ("dom", "rep")),
        ),
        out_specs=P(None, "dom", "rep", None),
        check_vma=False,
    )
```

```python
import functools

import jax
import jax.numpy as jnp
from jax import lax
from jax.experimental import pallas as pl
from jax.experimental.pallas import tpu as pltpu
from jax.sharding import PartitionSpec as P

HALF = 2
SLOTS = 3
HOOD = 2 * HALF + 2
MESH = pl.DeviceIdType.MESH
F32 = jnp.float32
BF16 = jnp.bfloat16


def iota(shape, dim):
    return lax.broadcasted_iota(jnp.int32, shape, dim).astype(F32)


def div(value, unit):
    return jnp.floor((value + 0.5) * (1.0 / unit))


def kernel(
    dims,
    src_hbm, dst_hbm, rs_hbm, diag_hbm, panel_hbm,
    out_ref,
    src_ref, dst_ref, rs_ref, small_sem,
    diag, panels_by_level, store, solved_ref, placed,
    slots_v, slots_s, slot_sem,
    val_send, val_recv, unpack, part_send, part_recv, id_send, id_recv,
    last_send, last_recv, last_unpack,
    diag_sem, panel_sem, val_ssem, val_rsem, part_ssem, part_rsem, id_ssem, id_rsem,
    last_ssem, last_rsem,
):
    levels, tiles, cols, width, panels, dom_size, rep_size, chunk = dims
    far = dom_size // 2
    block = rep_size // 2 * cols
    tile_rows = tiles * block
    rows = SLOTS * block
    pairs = 2 * HOOD
    senders = HOOD * rep_size
    half_rows = cols
    own_rows = tiles * cols
    last = levels - 2
    zero_tile = (levels - 1) * tiles
    me_d = lax.axis_index("dom")
    me_r = lax.axis_index("rep")
    my_half = lax.rem(me_r, 2)
    my_place = me_r // 2
    partner = me_r + 1 - 2 * my_half
    offsets = [o - HALF for o in range(HOOD - 1)] + [far]
    order = (HOOD - 1, 0, HOOD - 2, HALF, 1, HOOD - 3)
    groups = ((1, 3), (0, 4), (5, 2))

    def peer_dom(offset):
        return lax.rem(me_d + (offset + dom_size), dom_size)

    def peer_rep(step):
        return lax.rem(me_r + step, rep_size)

    peers = [(j, side) for j in order for side in (1, 0) if (offsets[j], side) != (0, 0)]
    others = list(range(1, rep_size))
    everyone = [(j, step) for j in order for step in others + [0] if (offsets[j], step) != (0, 0)]

    def load_diag(level):
        return pltpu.make_async_copy(diag_hbm.at[level], diag.at[level], diag_sem.at[level])

    def load_panel(level, part):
        span = pl.ds(part * chunk, chunk)
        return pltpu.make_async_copy(
            panel_hbm.at[level, span], panels_by_level[level].at[span], panel_sem.at[level, part]
        )

    def side_rep(side):
        return partner if side else me_r

    def side_half(side):
        return 1 - my_half if side else my_half

    def send_id(j, step):
        return pltpu.make_async_remote_copy(
            src_ref=id_send.at[j],
            dst_ref=id_recv.at[j, me_r],
            send_sem=id_ssem.at[j, step],
            recv_sem=id_rsem.at[j, me_r],
            device_id=(peer_dom(offsets[j]), peer_rep(step)),
            device_id_type=MESH,
        )

    def await_id(j, step):
        slot = peer_rep(step)
        pltpu.make_async_remote_copy(
            src_ref=id_send.at[j],
            dst_ref=id_recv.at[j, slot],
            send_sem=id_ssem.at[j, step],
            recv_sem=id_rsem.at[j, slot],
            device_id=(peer_dom(-offsets[j]), slot),
            device_id_type=MESH,
        ).wait_recv()

    def send_last(j, step):
        return pltpu.make_async_remote_copy(
            src_ref=last_send.at[j, peer_rep(step)],
            dst_ref=last_recv.at[j, me_r],
            send_sem=last_ssem.at[j, step],
            recv_sem=last_rsem.at[j, me_r],
            device_id=(peer_dom(offsets[j]), peer_rep(step)),
            device_id_type=MESH,
        )

    def await_last(j, step):
        slot = peer_rep(step)
        pltpu.make_async_remote_copy(
            src_ref=last_send.at[j, slot],
            dst_ref=last_recv.at[j, slot],
            send_sem=last_ssem.at[j, step],
            recv_sem=last_rsem.at[j, slot],
            device_id=(peer_dom(-offsets[j]), slot),
            device_id_type=MESH,
        ).wait_recv()

    def send_val(level, j, side):
        return pltpu.make_async_remote_copy(
            src_ref=val_send.at[level, side_half(side), j],
            dst_ref=val_recv.at[level, j, my_half],
            send_sem=val_ssem.at[level, j, side],
            recv_sem=val_rsem.at[level, j, my_half],
            device_id=(peer_dom(offsets[j]), side_rep(side)),
            device_id_type=MESH,
        )

    def await_val(level, j, side):
        pltpu.make_async_remote_copy(
            src_ref=val_send.at[level, side_half(side), j],
            dst_ref=val_recv.at[level, j, side_half(side)],
            send_sem=val_ssem.at[level, j, side],
            recv_sem=val_rsem.at[level, j, side_half(side)],
            device_id=(peer_dom(-offsets[j]), side_rep(side)),
            device_id_type=MESH,
        ).wait_recv()

    def part_span(level):
        return pl.ds(0, tile_rows if level else own_rows)

    def send_part(level, step):
        return pltpu.make_async_remote_copy(
            src_ref=part_send.at[level, part_span(level)],
            dst_ref=part_recv.at[level, me_r, part_span(level)],
            send_sem=part_ssem.at[level, step],
            recv_sem=part_rsem.at[level, me_r],
            device_id=(me_d, peer_rep(step)),
            device_id_type=MESH,
        )

    def await_part(level, step):
        slot = peer_rep(step)
        pltpu.make_async_remote_copy(
            src_ref=part_send.at[level, part_span(level)],
            dst_ref=part_recv.at[level, slot, part_span(level)],
            send_sem=part_ssem.at[level, step],
            recv_sem=part_rsem.at[level, slot],
            device_id=(me_d, slot),
            device_id_type=MESH,
        ).wait_recv()

    small = [
        pltpu.make_async_copy(hbm, ref, small_sem.at[i])
        for i, (hbm, ref) in enumerate(((rs_hbm, rs_ref), (dst_hbm, dst_ref), (src_hbm, src_ref)))
    ]
    for copy in small:
        copy.start()
    load_diag(0).start()
    for part in range(panels // chunk):
        load_panel(0, part).start()

    barrier = pltpu.get_barrier_semaphore()
    for j, step in everyone:
        pl.semaphore_signal(
            barrier,
            inc=1,
            device_id=(peer_dom(offsets[j]), peer_rep(step)),
            device_id_type=MESH,
        )

    def place(level):
        row = lax.broadcasted_iota(jnp.int32, (block, width), 0) // cols
        for t in range(tiles):
            twice = jnp.concatenate([rs_ref[level, t]] * (rep_size // 2), axis=0)
            placed[level, t * block : (t + 1) * block] = jnp.where(row == my_place, twice, 0.0)

    def share(level, partial):
        rounded = partial.astype(BF16)
        part_send[level, : rounded.shape[0]] = rounded
        for step in others:
            send_part(level, step).start()
        part_recv[level, me_r, : rounded.shape[0]] = rounded

    def route():
        owner = me_d.astype(F32)
        row16 = iota((panels, panels), 0)
        col16 = iota((panels, panels), 1)
        lane = iota((1, 128), 1)
        id_level = div(lane, rows)
        id_rest = lane - rows * id_level
        id_slot = div(id_rest, block)
        id_col = id_rest - block * id_slot
        panel_col = iota((panels, 1), 0)
        wanted = [jnp.zeros((1, 128), F32) for _ in range(HOOD)]
        for l in range(levels - 1):
            drow = dst_ref[l : l + 1, :].astype(F32)
            srow = src_ref[l : l + 1, :].astype(F32)
            dcol = jnp.sum(jnp.where(row16 == col16, drow, 0.0), axis=1, keepdims=True)
            scol = jnp.sum(jnp.where(row16 == col16, srow, 0.0), axis=1, keepdims=True)
            trow = jnp.where(drow >= 0, div(drow, tiles), -1.0)
            tcol = jnp.where(dcol >= 0, div(dcol, tiles), -1.0)
            earlier = (tcol == trow) & (drow >= 0) & (col16 < row16)
            rank = jnp.sum(jnp.where(earlier, 1.0, 0.0), axis=1, keepdims=True)
            away = tcol - owner
            away = away + jnp.where(away < 0, float(dom_size), 0.0)
            near = away + HALF
            near = near - jnp.where(near >= dom_size, float(dom_size), 0.0)
            reach = jnp.where(away == far, float(HOOD - 1), near)
            reach = jnp.where(dcol >= 0, reach, -1.0)
            spot = jnp.where(dcol >= 0, reach * SLOTS + rank, -1.0)
            tile = dcol - tiles * tcol
            here = spot == lane
            which = jnp.sum(jnp.where(here, panel_col, 0.0), axis=0, keepdims=True)
            source = jnp.sum(jnp.where(here, scol - zero_tile, 0.0), axis=0, keepdims=True)
            slots_v[2 * l : 2 * l + 1, :] = which.astype(jnp.int32)
            slots_v[2 * l + 1 : 2 * l + 2, :] = (source + zero_tile).astype(jnp.int32)
            if l == last:
                id_slot = div(id_rest, cols)
                id_col = id_rest - cols * id_slot
            mine = (rank == id_slot) & (id_level == l)
            for j in range(HOOD):
                spread = tile * (cols if l == last else block) + id_col + 1.0
                found = jnp.where(mine & (reach == j), spread, 0.0)
                wanted[j] = wanted[j] + jnp.sum(found, axis=0, keepdims=True)
        for j in range(HOOD):
            id_send[j] = (wanted[j] - 1.0).astype(jnp.int32)
        id_recv[HALF, me_r] = id_send[HALF]

    def learn_ids():
        for j, step in everyone:
            await_id(j, step)

        def lookup(ids, count, span, lane_in):
            lane_sender = div(iota((1, span), 1), span // count)
            take = jnp.where(iota((128, span), 0) == lane_in, 1.0, 0.0)
            every = jnp.dot(ids, take.astype(BF16), preferred_element_type=F32)
            own = jnp.where(iota((count, span), 0) == lane_sender, every, 0.0)
            return jnp.sum(own, axis=0, keepdims=True)

        near = jnp.zeros((pairs, 128), F32)
        full = jnp.zeros((senders, 128), F32)
        for j in range(HOOD):
            for side in range(2):
                row = id_recv[j, my_place * 2 + side].astype(F32)
                near = jnp.where(iota((pairs, 128), 0) == 2 * j + side, row, near)
            for r in range(rep_size):
                row = id_recv[j, r].astype(F32)
                full = jnp.where(iota((senders, 128), 0) == rep_size * j + r, row, full)
        span = pairs * rows
        lane = iota((1, span), 1)
        lane_in = lane - rows * div(lane, rows)
        for l in range(last):
            goal = lookup(near.astype(BF16), pairs, span, lane_in + l * rows)
            unpack[l] = jnp.where(iota((tile_rows, span), 0) == goal, 1.0, 0.0).astype(BF16)
        span = senders * half_rows
        lane = iota((1, span), 1)
        lane_in = lane - half_rows * div(lane, half_rows)
        full = full.astype(BF16)
        for i in range(SLOTS):
            goal = lookup(full, senders, span, lane_in + (last * rows + i * cols))
            last_unpack[i] = jnp.where(iota((own_rows, span), 0) == goal, 1.0, 0.0).astype(BF16)

    def emit(level):
        for t in range(tiles):
            mine = solved_ref[level, t, my_half]
            picked = mine[:cols]
            for q in range(1, rep_size // 2):
                picked = jnp.where(my_place == q, mine[q * cols : (q + 1) * cols], picked)
            out_ref[level, t] = picked

    def own_sides(level):
        return jnp.concatenate([rs_ref[level, t] for t in range(tiles)], axis=0)

    small[0].wait()
    pl.semaphore_wait(barrier, len(everyone))
    share(0, own_sides(0))
    small[1].wait()
    small[2].wait()
    route()
    slot_copy = pltpu.make_async_copy(slots_v, slots_s, slot_sem)
    slot_copy.start()
    for j, step in everyone:
        send_id(j, step).start()
    for level in range(1, levels - 1):
        place(level)
    store[zero_tile] = jnp.zeros((2 * block, width), BF16)

    for level in range(levels - 1):
        for step in others:
            await_part(level, step)
        if level == 0:
            parts = [part_recv[0, r, :own_rows].astype(F32) for r in range(rep_size)]
            residuals = [
                jnp.concatenate(
                    [
                        parts[r][t * cols : (t + 1) * cols]
                        for h in range(2)
                        for r in range(h, rep_size, 2)
                    ],
                    axis=0,
                )
                for t in range(tiles)
            ]
        else:
            halves = []
            for h in range(2):
                total = part_recv[level, h].astype(F32)
                for r in range(h + 2, rep_size, 2):
                    total = total + part_recv[level, r].astype(F32)
                halves.append(total)
            residuals = [
                jnp.concatenate([half[t * block : (t + 1) * block] for half in halves], axis=0)
                for t in range(tiles)
            ]
        load_diag(level).wait()
        for t in range(tiles):
            residual = residuals[t].astype(BF16)
            solved = jnp.dot(residual, diag[level, t], preferred_element_type=F32)
            store[level * tiles + t] = solved.astype(BF16)
            for h in range(2):
                solved_ref[level, t, h] = solved[h * block : (h + 1) * block]
        if level == 0:
            slot_copy.wait()
        for part in range(panels // chunk):
            load_panel(level, part).wait()
        for group in groups:
            products = {}
            for j in group:
                for k in range(SLOTS):
                    which = jnp.clip(slots_s[2 * level, j * SLOTS + k], 0, panels - 1)
                    source = jnp.clip(slots_s[2 * level + 1, j * SLOTS + k], 0, zero_tile)
                    products[j, k] = jnp.dot(
                        store[source], panels_by_level[level][which], preferred_element_type=F32
                    )
            for j in group:
                if level < last:
                    for k in range(SLOTS):
                        rounded = products[j, k].astype(BF16)
                        for h in range(2):
                            val_send[level, h, j, k * block : (k + 1) * block] = rounded[
                                h * block : (h + 1) * block
                            ]
                else:
                    for r in range(rep_size):
                        begin = r % 2 * block + r // 2 * cols
                        piece = [products[j, k][begin : begin + cols] for k in range(SLOTS)]
                        for k in range(SLOTS):
                            last_send[j, r, :, k * width : (k + 1) * width] = piece[k].astype(BF16)
            if level < last:
                for side in (1, 0):
                    for j in group:
                        if (j, side) in peers:
                            send_val(level, j, side).start()
            else:
                for step in others + [0]:
                    for j in group:
                        if (j, step) in everyone:
                            send_last(j, step).start()
        if level < last:
            val_recv[level, HALF, my_half] = val_send[level, my_half, HALF]
        else:
            last_recv[HALF, me_r] = last_send[HALF, me_r]
        load_diag(level + 1).start()
        if level < last:
            for part in range(panels // chunk):
                load_panel(level + 1, part).start()
        if level == 0:
            learn_ids()
        emit(level)
        if level < last:
            for j, side in peers:
                await_val(level, j, side)
            arrived = val_recv[level].reshape(pairs * rows, width)
            incoming = jnp.dot(unpack[level], arrived, preferred_element_type=F32)
            share(level + 1, placed[level + 1] - incoming)

    for j, step in everyone:
        await_last(j, step)
    arrived = last_recv[...].reshape(senders * half_rows, SLOTS * width)
    residual = own_sides(levels - 1)
    for i in range(SLOTS):
        residual = residual - jnp.dot(
            last_unpack[i], arrived[:, i * width : (i + 1) * width], preferred_element_type=F32
        )
    residual = residual.astype(BF16)
    load_diag(levels - 1).wait()
    for t in range(tiles):
        solved = jnp.dot(residual, diag[levels - 1, t], preferred_element_type=F32)
        out_ref[levels - 1, t] = solved[t * cols : (t + 1) * cols]

    for j, step in everyone:
        send_id(j, step).wait_send()
        send_last(j, step).wait_send()
    for j, side in peers:
        for level in range(last):
            send_val(level, j, side).wait_send()
    for step in others:
        for level in range(levels - 1):
            send_part(level, step).wait_send()


def per_device(right_sides, diag_inverse, panel_mats, panel_src, panel_dst):
    levels, tiles, cols, width = right_sides.shape
    panels = panel_mats.shape[1]
    dom_size = lax.axis_size("dom")
    rep_size = lax.axis_size("rep")
    block = rep_size // 2 * cols
    tile_rows = tiles * block
    rows = SLOTS * block
    chunk = 4 if panels % 4 == 0 else 1
    assert rep_size % 2 == 0 and block % 8 == 0 and (levels - 1) * rows <= 128
    assert 2 * cols == 8 and width % 384 == 0 and levels > 2
    dims = (levels, tiles, cols, width, panels, dom_size, rep_size, chunk)
    vmem = pl.BlockSpec(memory_space=pltpu.VMEM)
    hbm = pl.BlockSpec(memory_space=pl.ANY)
    dma = pltpu.SemaphoreType.DMA
    i32 = jnp.int32
    return pl.pallas_call(
        functools.partial(kernel, dims),
        out_shape=jax.ShapeDtypeStruct(right_sides.shape, F32),
        in_specs=[hbm] * 5,
        out_specs=vmem,
        scratch_shapes=[
            pltpu.VMEM(panel_src.shape, i32),
            pltpu.VMEM(panel_dst.shape, i32),
            pltpu.VMEM(right_sides.shape, F32),
            dma((3,)),
            pltpu.VMEM(diag_inverse.shape, BF16),
            [pltpu.VMEM(panel_mats.shape[1:], BF16) for _ in range(levels - 1)],
            pltpu.VMEM(((levels - 1) * tiles + 1, 2 * block, width), BF16),
            pltpu.VMEM((levels - 1, tiles, 2, block, width), F32),
            pltpu.VMEM((levels - 1, tile_rows, width), F32),
            pltpu.VMEM((8, 128), i32),
            pltpu.SMEM((8, 128), i32),
            dma,
            pltpu.VMEM((levels - 2, 2, HOOD, rows, width), BF16),
            pltpu.VMEM((levels - 2, HOOD, 2, rows, width), BF16),
            pltpu.VMEM((levels - 2, tile_rows, 2 * HOOD * rows), BF16),
            pltpu.VMEM((levels - 1, tile_rows, width), BF16),
            pltpu.VMEM((levels - 1, rep_size, tile_rows, width), BF16),
            pltpu.VMEM((HOOD, 1, 128), i32),
            pltpu.VMEM((HOOD, rep_size, 1, 128), i32),
            pltpu.VMEM((HOOD, rep_size, cols, SLOTS * width), BF16),
            pltpu.VMEM((HOOD, rep_size, cols, SLOTS * width), BF16),
            pltpu.VMEM((SLOTS, tiles * cols, HOOD * rep_size * cols), BF16),
            dma((levels,)),
            dma((levels - 1, panels // chunk)),
            dma((levels - 2, HOOD, 2)),
            dma((levels - 2, HOOD, 2)),
            dma((levels - 1, rep_size)),
            dma((levels - 1, rep_size)),
            dma((HOOD, rep_size)),
            dma((HOOD, rep_size)),
            dma((HOOD, rep_size)),
            dma((HOOD, rep_size)),
        ],
        compiler_params=pltpu.CompilerParams(
            collective_id=0, has_side_effects=True, vmem_limit_bytes=67043328
        ),
    )(panel_src, panel_dst, right_sides, diag_inverse, panel_mats)


def solution(mesh):
    return jax.shard_map(
        per_device,
        mesh=mesh,
        in_specs=(
            P(None, "dom", "rep", None),
            P(None, "dom", None, None),
            P(None, ("dom", "rep"), None, None),
            P(None, ("dom", "rep")),
            P(None, ("dom", "rep")),
        ),
        out_specs=P(None, "dom", "rep", None),
        check_vma=False,
    )
```

```python
import functools

import jax
import jax.numpy as jnp
from jax import lax
from jax.experimental import pallas as pl
from jax.experimental.pallas import tpu as pltpu
from jax.sharding import PartitionSpec as P

HALF = 2
SLOTS = 3
HOOD = 2 * HALF + 2
MESH = pl.DeviceIdType.MESH
F32 = jnp.float32
BF16 = jnp.bfloat16


def iota(shape, dim):
    return lax.broadcasted_iota(jnp.int32, shape, dim).astype(F32)


def div(value, unit):
    return jnp.floor((value + 0.5) * (1.0 / unit))


def kernel(
    dims,
    src_hbm, dst_hbm, rs_hbm, diag_hbm, panel_hbm,
    out_ref,
    src_ref, dst_ref, rs_ref, small_sem,
    diag, panels_by_level, store, solved_ref, placed,
    slots_v, slots_s, slot_sem,
    val_send, val_recv, unpack, part_send, part_recv, id_send, id_recv,
    unit_send, unit_recv, unit_unpack, last_send, last_recv,
    diag_sem, panel_sem, val_ssem, val_rsem, part_ssem, part_rsem, id_ssem, id_rsem,
    unit_ssem, unit_rsem, last_ssem, last_rsem,
):
    levels, tiles, cols, width, panels, dom_size, rep_size, chunk = dims
    far = dom_size // 2
    block = rep_size // 2 * cols
    tile_rows = tiles * block
    rows = SLOTS * block
    pairs = 2 * HOOD
    senders = HOOD * rep_size
    half_rows = cols
    own_rows = tiles * cols
    last = levels - 2
    zero_tile = (levels - 1) * tiles
    me_d = lax.axis_index("dom")
    me_r = lax.axis_index("rep")
    ends, inner = (0, rep_size - 1), (1, rep_size - 2)
    ranking = ends + inner
    my_side = me_r // 2
    my_end = my_side * (rep_size - 1)
    my_turn = lax.rem(me_r, 2)
    my_unit = lax.rem(me_r + 1, 2)
    my_half = lax.rem((me_r + 1) // 2, 2)
    is_end = my_half == 0
    is_inner = my_half == 1
    offsets = [o - HALF for o in range(HOOD - 1)] + [far]
    order = (HOOD - 1, 0, HOOD - 2, HALF, 1, HOOD - 3)
    val_groups = ((1, 3), (0, 4), (2, 5))
    last_groups = ((0, 4), (1, 3), (5, 2))

    def peer_dom(offset):
        return lax.rem(me_d + (offset + dom_size), dom_size)

    def peer_rep(step):
        return lax.rem(me_r + step, rep_size)

    others = list(range(1, rep_size))
    everyone = [(j, step) for j in order for step in others + [0] if (offsets[j], step) != (0, 0)]

    def load_diag(level):
        return pltpu.make_async_copy(diag_hbm.at[level], diag.at[level], diag_sem.at[level])

    def load_panel(level, part):
        span = pl.ds(part * chunk, chunk)
        return pltpu.make_async_copy(
            panel_hbm.at[level, span], panels_by_level[level].at[span], panel_sem.at[level, part]
        )

    def aim(step):
        if step == 0:
            return me_r
        end_aim = jnp.where(me_r == 0, rep_size - step, step - 1)
        inner_aim = ((rep_size - 1 - my_end, rep_size - 1 - me_r, my_end)[step - 1])
        return jnp.where(is_end, end_aim, inner_aim)

    def send_id(j, step):
        return pltpu.make_async_remote_copy(
            src_ref=id_send.at[j],
            dst_ref=id_recv.at[j, me_r],
            send_sem=id_ssem.at[j, step],
            recv_sem=id_rsem.at[j, me_r],
            device_id=(peer_dom(offsets[j]), peer_rep(step)),
            device_id_type=MESH,
        )

    def await_id(j, step):
        slot = peer_rep(step)
        pltpu.make_async_remote_copy(
            src_ref=id_send.at[j],
            dst_ref=id_recv.at[j, slot],
            send_sem=id_ssem.at[j, step],
            recv_sem=id_rsem.at[j, slot],
            device_id=(peer_dom(-offsets[j]), slot),
            device_id_type=MESH,
        ).wait_recv()

    def send_last(j, step):
        return pltpu.make_async_remote_copy(
            src_ref=last_send.at[j, peer_rep(step)],
            dst_ref=last_recv.at[j, me_r],
            send_sem=last_ssem.at[j, step],
            recv_sem=last_rsem.at[j, me_r],
            device_id=(peer_dom(offsets[j]), peer_rep(step)),
            device_id_type=MESH,
        )

    def await_last(j, step):
        slot = peer_rep(step)
        pltpu.make_async_remote_copy(
            src_ref=last_send.at[j, slot],
            dst_ref=last_recv.at[j, slot],
            send_sem=last_ssem.at[j, step],
            recv_sem=last_rsem.at[j, slot],
            device_id=(peer_dom(-offsets[j]), slot),
            device_id_type=MESH,
        ).wait_recv()

    def send_val(level, j):
        return pltpu.make_async_remote_copy(
            src_ref=val_send.at[level, j],
            dst_ref=val_recv.at[level, j, my_turn],
            send_sem=val_ssem.at[level, j],
            recv_sem=val_rsem.at[level, j, my_turn],
            device_id=(peer_dom(offsets[j]), my_end),
            device_id_type=MESH,
        )

    def await_val(level, j, other):
        turn = 1 - my_turn if other else my_turn
        pltpu.make_async_remote_copy(
            src_ref=val_send.at[level, j],
            dst_ref=val_recv.at[level, j, turn],
            send_sem=val_ssem.at[level, j],
            recv_sem=val_rsem.at[level, j, turn],
            device_id=(peer_dom(-offsets[j]), 2 * my_side + turn),
            device_id_type=MESH,
        ).wait_recv()

    def send_unit(level, j, m):
        return pltpu.make_async_remote_copy(
            src_ref=unit_send.at[level, j, m],
            dst_ref=unit_recv.at[level, j, me_r],
            send_sem=unit_ssem.at[level, j, m],
            recv_sem=unit_rsem.at[level, j, me_r],
            device_id=(peer_dom(offsets[j]), jnp.int32(inner[m])),
            device_id_type=MESH,
        )

    def await_unit(level, j, step):
        slot = peer_rep(step)
        pltpu.make_async_remote_copy(
            src_ref=unit_send.at[level, j, 0],
            dst_ref=unit_recv.at[level, j, slot],
            send_sem=unit_ssem.at[level, j, 0],
            recv_sem=unit_rsem.at[level, j, slot],
            device_id=(peer_dom(-offsets[j]), slot),
            device_id_type=MESH,
        ).wait_recv()

    def each_val(level, group, act):
        for j in group:
            for m in range(2):
                if offsets[j] != 0:
                    act(send_unit(level, j, m))
                else:
                    pl.when(me_r != inner[m])(lambda: act(send_unit(level, j, m)))
        for j in group:
            if offsets[j] != 0:
                act(send_val(level, j))
            else:
                pl.when(is_inner)(lambda: act(send_val(level, j)))

    def send_part(level, step, count):
        return pltpu.make_async_remote_copy(
            src_ref=part_send.at[level, pl.ds(0, count)],
            dst_ref=part_recv.at[level, me_r, pl.ds(0, count)],
            send_sem=part_ssem.at[level, step],
            recv_sem=part_rsem.at[level, me_r],
            device_id=(me_d, aim(step)),
            device_id_type=MESH,
        )

    def await_part(level, rep, count):
        pltpu.make_async_remote_copy(
            src_ref=part_send.at[level, pl.ds(0, count)],
            dst_ref=part_recv.at[level, rep, pl.ds(0, count)],
            send_sem=part_ssem.at[level, 1],
            recv_sem=part_rsem.at[level, rep],
            device_id=(me_d, jnp.int32(rep)),
            device_id_type=MESH,
        ).wait_recv()

    def count_of(level, rep):
        return tile_rows if level and rep in ends else own_rows

    small = [
        pltpu.make_async_copy(hbm, ref, small_sem.at[i])
        for i, (hbm, ref) in enumerate(((rs_hbm, rs_ref), (dst_hbm, dst_ref), (src_hbm, src_ref)))
    ]
    for copy in small:
        copy.start()
    load_diag(0).start()
    for part in range(panels // chunk):
        load_panel(0, part).start()

    barrier = pltpu.get_barrier_semaphore()
    for j, step in everyone:
        pl.semaphore_signal(
            barrier,
            inc=1,
            device_id=(peer_dom(offsets[j]), peer_rep(step)),
            device_id_type=MESH,
        )

    def place(level):
        row = lax.broadcasted_iota(jnp.int32, (block, width), 0) // cols
        for t in range(tiles):
            twice = jnp.concatenate([rs_ref[level, t]] * (rep_size // 2), axis=0)
            placed[level, t * block : (t + 1) * block] = jnp.where(row == my_side, twice, 0.0)

    def share(level, partial):
        rounded = partial.astype(BF16)
        count = rounded.shape[0]
        part_send[level, :count] = rounded
        for step in others:
            send_part(level, step, count).start()
        part_recv[level, me_r, :count] = rounded

    def route():
        owner = me_d.astype(F32)
        row16 = iota((panels, panels), 0)
        col16 = iota((panels, panels), 1)
        lane = iota((1, 128), 1)
        id_level = div(lane, SLOTS)
        id_slot = lane - SLOTS * id_level
        panel_col = iota((panels, 1), 0)
        wanted = [jnp.zeros((1, 128), F32) for _ in range(HOOD)]
        for l in range(levels - 1):
            drow = dst_ref[l : l + 1, :].astype(F32)
            srow = src_ref[l : l + 1, :].astype(F32)
            dcol = jnp.sum(jnp.where(row16 == col16, drow, 0.0), axis=1, keepdims=True)
            scol = jnp.sum(jnp.where(row16 == col16, srow, 0.0), axis=1, keepdims=True)
            trow = jnp.where(drow >= 0, div(drow, tiles), -1.0)
            tcol = jnp.where(dcol >= 0, div(dcol, tiles), -1.0)
            earlier = (tcol == trow) & (drow >= 0) & (col16 < row16)
            rank = jnp.sum(jnp.where(earlier, 1.0, 0.0), axis=1, keepdims=True)
            away = tcol - owner
            away = away + jnp.where(away < 0, float(dom_size), 0.0)
            near = away + HALF
            near = near - jnp.where(near >= dom_size, float(dom_size), 0.0)
            reach = jnp.where(away == far, float(HOOD - 1), near)
            reach = jnp.where(dcol >= 0, reach, -1.0)
            spot = jnp.where(dcol >= 0, reach * SLOTS + rank, -1.0)
            tile = dcol - tiles * tcol
            here = spot == lane
            which = jnp.sum(jnp.where(here, panel_col, 0.0), axis=0, keepdims=True)
            source = jnp.sum(jnp.where(here, scol - zero_tile, 0.0), axis=0, keepdims=True)
            slots_v[2 * l : 2 * l + 1, :] = which.astype(jnp.int32)
            slots_v[2 * l + 1 : 2 * l + 2, :] = (source + zero_tile).astype(jnp.int32)
            mine = (rank == id_slot) & (id_level == l)
            for j in range(HOOD):
                found = jnp.where(mine & (reach == j), tile + 1.0, 0.0)
                wanted[j] = wanted[j] + jnp.sum(found, axis=0, keepdims=True)
        for j in range(HOOD):
            id_send[j] = (wanted[j] - 1.0).astype(jnp.int32)
        id_recv[HALF, me_r] = id_send[HALF]

    def learn_ids():
        for j, step in everyone:
            await_id(j, step)

        def lookup(ids, count, span, lane_in):
            lane_sender = div(iota((1, span), 1), span // count)
            take = jnp.where(iota((128, span), 0) == lane_in, 1.0, 0.0)
            every = jnp.dot(ids, take.astype(BF16), preferred_element_type=F32)
            own = jnp.where(iota((count, span), 0) == lane_sender, every, 0.0)
            return jnp.sum(own, axis=0, keepdims=True)

        near = jnp.zeros((pairs, 128), F32)
        full = jnp.zeros((senders, 128), F32)
        for j in range(HOOD):
            for turn in range(2):
                row = id_recv[j, 2 * my_side + turn].astype(F32)
                near = jnp.where(iota((pairs, 128), 0) == 2 * j + turn, row, near)
            for r in range(rep_size):
                row = id_recv[j, r].astype(F32)
                full = jnp.where(iota((senders, 128), 0) == rep_size * j + r, row, full)
        near, full = near.astype(BF16), full.astype(BF16)
        span = pairs * rows
        lane = iota((1, span), 1)
        lane_in = lane - rows * div(lane, rows)
        lane_slot = div(lane_in, block)
        lane_col = lane_in - block * lane_slot
        for l in range(last):
            tile = lookup(near, pairs, span, lane_slot + l * SLOTS)
            goal = jnp.where(tile >= 0, tile * block + lane_col, -1.0)
            unpack[l] = jnp.where(iota((tile_rows, span), 0) == goal, 1.0, 0.0).astype(BF16)
        span = senders * cols
        lane = iota((1, span), 1)
        lane_col = lane - cols * div(lane, cols)
        for l in range(levels - 1):
            for k in range(SLOTS):
                tile = lookup(full, senders, span, jnp.full((1, span), float(l * SLOTS + k), F32))
                goal = jnp.where(tile >= 0, tile * cols + lane_col, -1.0)
                unit_unpack[l, k] = jnp.where(iota((own_rows, span), 0) == goal, 1.0, 0.0).astype(BF16)

    def gather_units(level, arrived):
        residual = own_sides(level + 1)
        arrived = arrived.reshape(senders * cols, SLOTS * width)
        for k in range(SLOTS):
            residual = residual - jnp.dot(
                unit_unpack[level, k],
                arrived[:, k * width : (k + 1) * width],
                preferred_element_type=F32,
            )
        return residual

    def emit(level):
        for t in range(tiles):
            mine = solved_ref[level, t, my_half]
            picked = mine[:cols]
            for q in range(1, rep_size // 2):
                picked = jnp.where(my_side == q, mine[q * cols : (q + 1) * cols], picked)
            out_ref[level, t] = picked

    def own_sides(level):
        return jnp.concatenate([rs_ref[level, t] for t in range(tiles)], axis=0)

    small[0].wait()
    pl.semaphore_wait(barrier, len(everyone))
    share(0, own_sides(0))
    small[1].wait()
    small[2].wait()
    route()
    slot_copy = pltpu.make_async_copy(slots_v, slots_s, slot_sem)
    slot_copy.start()
    for j, step in everyone:
        send_id(j, step).start()
    for level in range(1, levels - 1):
        place(level)
    store[zero_tile] = jnp.zeros((2 * block, width), BF16)

    for level in range(levels - 1):
        for r in range(rep_size):
            pl.when(me_r != r)(lambda: await_part(level, r, count_of(level, r)))
        if level == 0:
            parts = [part_recv[0, r, :own_rows].astype(F32) for r in range(rep_size)]
            residuals = [
                jnp.concatenate(
                    [parts[r][t * cols : (t + 1) * cols] for r in ranking], axis=0
                )
                for t in range(tiles)
            ]
        else:
            total = part_recv[level, ends[0]].astype(F32) + part_recv[level, ends[1]].astype(F32)
            parts = [part_recv[level, r, :own_rows].astype(F32) for r in inner]
            residuals = [
                jnp.concatenate(
                    [total[t * block : (t + 1) * block]]
                    + [part[t * cols : (t + 1) * cols] for part in parts],
                    axis=0,
                )
                for t in range(tiles)
            ]
        load_diag(level).wait()
        for t in range(tiles):
            residual = residuals[t].astype(BF16)
            solved = jnp.dot(residual, diag[level, t], preferred_element_type=F32)
            store[level * tiles + t] = solved.astype(BF16)
            for h in range(2):
                solved_ref[level, t, h] = solved[h * block : (h + 1) * block]
        if level == 0:
            slot_copy.wait()
        for part in range(panels // chunk):
            load_panel(level, part).wait()
        for group in val_groups if level < last else last_groups:
            products = {}
            for j in group:
                for k in range(SLOTS):
                    which = jnp.clip(slots_s[2 * level, j * SLOTS + k], 0, panels - 1)
                    source = jnp.clip(slots_s[2 * level + 1, j * SLOTS + k], 0, zero_tile)
                    products[j, k] = jnp.dot(
                        store[source], panels_by_level[level][which], preferred_element_type=F32
                    )
            for j in group:
                if level < last:
                    for k in range(SLOTS):
                        rounded = products[j, k].astype(BF16)
                        val_send[level, j, k * block : (k + 1) * block] = rounded[:block]
                        for m in range(2):
                            begin = block + m * cols
                            unit_send[level, j, m, :, k * width : (k + 1) * width] = products[j, k][
                                begin : begin + cols
                            ].astype(BF16)
                else:
                    for r in range(rep_size):
                        begin = ranking.index(r) * cols
                        piece = [products[j, k][begin : begin + cols] for k in range(SLOTS)]
                        for k in range(SLOTS):
                            last_send[j, r, :, k * width : (k + 1) * width] = piece[k].astype(BF16)
            if level < last:
                each_val(level, group, lambda copy: copy.start())
            else:
                for step in others + [0]:
                    for j in group:
                        if (j, step) in everyone:
                            send_last(j, step).start()
        if level < last:

            @pl.when(is_end)
            def _():
                val_recv[level, HALF, my_turn] = val_send[level, HALF]

            @pl.when(is_inner)
            def _():
                unit_recv[level, HALF, me_r] = unit_send[level, HALF, my_unit]

        else:
            last_recv[HALF, me_r] = last_send[HALF, me_r]
        load_diag(level + 1).start()
        if level < last:
            for part in range(panels // chunk):
                load_panel(level + 1, part).start()
        if level == 0:
            learn_ids()
        emit(level)
        if level < last:

            @pl.when(is_end)
            def _():
                for j in order:
                    for other in (True, False):
                        if other or offsets[j] != 0:
                            await_val(level, j, other)
                arrived = val_recv[level].reshape(pairs * rows, width)
                incoming = jnp.dot(unpack[level], arrived, preferred_element_type=F32)
                share(level + 1, placed[level + 1] - incoming)

            @pl.when(is_inner)
            def _():
                for j, step in everyone:
                    await_unit(level, j, step)
                share(level + 1, gather_units(level, unit_recv[level]))

    for j, step in everyone:
        await_last(j, step)
    residual = gather_units(last, last_recv[...])
    residual = residual.astype(BF16)
    load_diag(levels - 1).wait()
    for t in range(tiles):
        solved = jnp.dot(residual, diag[levels - 1, t], preferred_element_type=F32)
        out_ref[levels - 1, t] = solved[t * cols : (t + 1) * cols]

    for j, step in everyone:
        send_id(j, step).wait_send()
        send_last(j, step).wait_send()
    for level in range(last):
        each_val(level, order, lambda copy: copy.wait_send())
    for step in others:
        send_part(0, step, own_rows).wait_send()
        for level in range(1, levels - 1):
            pl.when(is_end)(lambda: send_part(level, step, tile_rows).wait_send())
            pl.when(is_inner)(lambda: send_part(level, step, own_rows).wait_send())


def per_device(right_sides, diag_inverse, panel_mats, panel_src, panel_dst):
    levels, tiles, cols, width = right_sides.shape
    panels = panel_mats.shape[1]
    dom_size = lax.axis_size("dom")
    rep_size = lax.axis_size("rep")
    block = rep_size // 2 * cols
    tile_rows = tiles * block
    rows = SLOTS * block
    chunk = 4 if panels % 4 == 0 else 1
    assert rep_size == 4 and block % 8 == 0 and (levels - 1) * SLOTS <= 128 and levels > 2
    dims = (levels, tiles, cols, width, panels, dom_size, rep_size, chunk)
    vmem = pl.BlockSpec(memory_space=pltpu.VMEM)
    hbm = pl.BlockSpec(memory_space=pl.ANY)
    dma = pltpu.SemaphoreType.DMA
    i32 = jnp.int32
    return pl.pallas_call(
        functools.partial(kernel, dims),
        out_shape=jax.ShapeDtypeStruct(right_sides.shape, F32),
        in_specs=[hbm] * 5,
        out_specs=vmem,
        scratch_shapes=[
            pltpu.VMEM(panel_src.shape, i32),
            pltpu.VMEM(panel_dst.shape, i32),
            pltpu.VMEM(right_sides.shape, F32),
            dma((3,)),
            pltpu.VMEM(diag_inverse.shape, BF16),
            [pltpu.VMEM(panel_mats.shape[1:], BF16) for _ in range(levels - 1)],
            pltpu.VMEM(((levels - 1) * tiles + 1, 2 * block, width), BF16),
            pltpu.VMEM((levels - 1, tiles, 2, block, width), F32),
            pltpu.VMEM((levels - 1, tile_rows, width), F32),
            pltpu.VMEM((8, 128), i32),
            pltpu.SMEM((8, 128), i32),
            dma,
            pltpu.VMEM((levels - 2, HOOD, rows, width), BF16),
            pltpu.VMEM((levels - 2, HOOD, 2, rows, width), BF16),
            pltpu.VMEM((levels - 2, tile_rows, 2 * HOOD * rows), BF16),
            pltpu.VMEM((levels - 1, tile_rows, width), BF16),
            pltpu.VMEM((levels - 1, rep_size, tile_rows, width), BF16),
            pltpu.VMEM((HOOD, 1, 128), i32),
            pltpu.VMEM((HOOD, rep_size, 1, 128), i32),
            pltpu.VMEM((levels - 2, HOOD, 2, cols, SLOTS * width), BF16),
            pltpu.VMEM((levels - 2, HOOD, rep_size, cols, SLOTS * width), BF16),
            pltpu.VMEM((levels - 1, SLOTS, tiles * cols, HOOD * rep_size * cols), BF16),
            pltpu.VMEM((HOOD, rep_size, cols, SLOTS * width), BF16),
            pltpu.VMEM((HOOD, rep_size, cols, SLOTS * width), BF16),
            dma((levels,)),
            dma((levels - 1, panels // chunk)),
            dma((levels - 2, HOOD)),
            dma((levels - 2, HOOD, 2)),
            dma((levels - 1, rep_size)),
            dma((levels - 1, rep_size)),
            dma((HOOD, rep_size)),
            dma((HOOD, rep_size)),
            dma((levels - 2, HOOD, 2)),
            dma((levels - 2, HOOD, rep_size)),
            dma((HOOD, rep_size)),
            dma((HOOD, rep_size)),
        ],
        compiler_params=pltpu.CompilerParams(
            collective_id=0, has_side_effects=True, vmem_limit_bytes=67043328
        ),
    )(panel_src, panel_dst, right_sides, diag_inverse, panel_mats)


def solution(mesh):
    return jax.shard_map(
        per_device,
        mesh=mesh,
        in_specs=(
            P(None, "dom", "rep", None),
            P(None, "dom", None, None),
            P(None, ("dom", "rep"), None, None),
            P(None, ("dom", "rep")),
            P(None, ("dom", "rep")),
        ),
        out_specs=P(None, "dom", "rep", None),
        check_vma=False,
    )
```

```python
import functools

import jax
import jax.numpy as jnp
from jax import lax
from jax.experimental import pallas as pl
from jax.experimental.pallas import tpu as pltpu
from jax.sharding import PartitionSpec as P

HALF = 2
SLOTS = 3
HOOD = 2 * HALF + 2
MESH = pl.DeviceIdType.MESH
F32 = jnp.float32
BF16 = jnp.bfloat16


def iota(shape, dim):
    return lax.broadcasted_iota(jnp.int32, shape, dim).astype(F32)


def div(value, unit):
    return jnp.floor((value + 0.5) * (1.0 / unit))


def kernel(
    dims,
    src_hbm, dst_hbm, rs_hbm, diag_hbm, panel_hbm,
    out_ref,
    src_ref, dst_ref, rs_ref, small_sem,
    diag, panels_by_level, store, solved_ref, placed,
    slots_v, slots_s, slot_sem,
    val_send, val_recv, unpack, part_send, part_recv, id_send, id_recv,
    unit_send, unit_recv, unit_unpack, last_send, last_recv,
    diag_sem, panel_sem, val_ssem, val_rsem, part_ssem, part_rsem, id_ssem, id_rsem,
    unit_ssem, unit_rsem, last_ssem, last_rsem,
):
    levels, tiles, cols, width, panels, dom_size, rep_size, chunk = dims
    far = dom_size // 2
    block = rep_size // 2 * cols
    tile_rows = tiles * block
    rows = SLOTS * block
    pairs = 2 * HOOD
    senders = HOOD * rep_size
    half_rows = cols
    own_rows = tiles * cols
    last = levels - 2
    zero_tile = (levels - 1) * tiles
    me_d = lax.axis_index("dom")
    me_r = lax.axis_index("rep")
    ends, inner = (0, rep_size - 1), (1, rep_size - 2)
    ranking = ends + inner
    my_side = me_r // 2
    my_end = my_side * (rep_size - 1)
    my_turn = lax.rem(me_r, 2)
    my_unit = lax.rem(me_r + 1, 2)
    my_half = lax.rem((me_r + 1) // 2, 2)
    is_end = my_half == 0
    is_inner = my_half == 1
    offsets = [o - HALF for o in range(HOOD - 1)] + [far]
    order = (HOOD - 1, 0, HOOD - 2, HALF, 1, HOOD - 3)
    val_groups = ((1, 3), (0, 4), (2, 5))
    last_groups = ((0, 4), (1, 3), (5, 2))

    def peer_dom(offset):
        return lax.rem(me_d + (offset + dom_size), dom_size)

    def peer_rep(step):
        return lax.rem(me_r + step, rep_size)

    others = list(range(1, rep_size))
    everyone = [(j, step) for j in order for step in others + [0] if (offsets[j], step) != (0, 0)]

    def load_diag(level):
        return pltpu.make_async_copy(diag_hbm.at[level], diag.at[level], diag_sem.at[level])

    def load_panel(level, part):
        span = pl.ds(part * chunk, chunk)
        return pltpu.make_async_copy(
            panel_hbm.at[level, span], panels_by_level[level].at[span], panel_sem.at[level, part]
        )

    def aim(step):
        if step == 0:
            return me_r
        end_aim = jnp.where(me_r == 0, rep_size - step, step - 1)
        inner_aim = ((rep_size - 1 - my_end, rep_size - 1 - me_r, my_end)[step - 1])
        return jnp.where(is_end, end_aim, inner_aim)

    def send_id(j, step):
        return pltpu.make_async_remote_copy(
            src_ref=id_send.at[j],
            dst_ref=id_recv.at[j, me_r],
            send_sem=id_ssem.at[j, step],
            recv_sem=id_rsem.at[j, me_r],
            device_id=(peer_dom(offsets[j]), peer_rep(step)),
            device_id_type=MESH,
        )

    def await_id(j, step):
        slot = peer_rep(step)
        pltpu.make_async_remote_copy(
            src_ref=id_send.at[j],
            dst_ref=id_recv.at[j, slot],
            send_sem=id_ssem.at[j, step],
            recv_sem=id_rsem.at[j, slot],
            device_id=(peer_dom(-offsets[j]), slot),
            device_id_type=MESH,
        ).wait_recv()

    def send_last(j, step):
        return pltpu.make_async_remote_copy(
            src_ref=last_send.at[j, peer_rep(step)],
            dst_ref=last_recv.at[j, me_r],
            send_sem=last_ssem.at[j, step],
            recv_sem=last_rsem.at[j, me_r],
            device_id=(peer_dom(offsets[j]), peer_rep(step)),
            device_id_type=MESH,
        )

    def await_last(j, step):
        slot = peer_rep(step)
        pltpu.make_async_remote_copy(
            src_ref=last_send.at[j, slot],
            dst_ref=last_recv.at[j, slot],
            send_sem=last_ssem.at[j, step],
            recv_sem=last_rsem.at[j, slot],
            device_id=(peer_dom(-offsets[j]), slot),
            device_id_type=MESH,
        ).wait_recv()

    def send_val(level, j):
        return pltpu.make_async_remote_copy(
            src_ref=val_send.at[level, j],
            dst_ref=val_recv.at[level, j, my_turn],
            send_sem=val_ssem.at[level, j],
            recv_sem=val_rsem.at[level, j, my_turn],
            device_id=(peer_dom(offsets[j]), my_end),
            device_id_type=MESH,
        )

    def await_val(level, j, other):
        turn = 1 - my_turn if other else my_turn
        pltpu.make_async_remote_copy(
            src_ref=val_send.at[level, j],
            dst_ref=val_recv.at[level, j, turn],
            send_sem=val_ssem.at[level, j],
            recv_sem=val_rsem.at[level, j, turn],
            device_id=(peer_dom(-offsets[j]), 2 * my_side + turn),
            device_id_type=MESH,
        ).wait_recv()

    def send_unit(level, j, m):
        target = 1 - my_side if m else my_side
        return pltpu.make_async_remote_copy(
            src_ref=unit_send.at[level, j, target],
            dst_ref=unit_recv.at[level, j, me_r],
            send_sem=unit_ssem.at[level, j, m],
            recv_sem=unit_rsem.at[level, j, me_r],
            device_id=(peer_dom(offsets[j]), 1 + target),
            device_id_type=MESH,
        )

    def await_unit(level, j, step):
        slot = peer_rep(step)
        pltpu.make_async_remote_copy(
            src_ref=unit_send.at[level, j, 0],
            dst_ref=unit_recv.at[level, j, slot],
            send_sem=unit_ssem.at[level, j, 0],
            recv_sem=unit_rsem.at[level, j, slot],
            device_id=(peer_dom(-offsets[j]), slot),
            device_id_type=MESH,
        ).wait_recv()

    def each_val(level, group, act):
        for j in group:
            act(send_unit(level, j, 1))
        for j in group:
            if offsets[j] != 0:
                act(send_unit(level, j, 0))
            else:
                pl.when(is_end)(lambda: act(send_unit(level, j, 0)))
        for j in group:
            if offsets[j] != 0:
                act(send_val(level, j))
            else:
                pl.when(is_inner)(lambda: act(send_val(level, j)))

    def send_part(level, step, count):
        return pltpu.make_async_remote_copy(
            src_ref=part_send.at[level, pl.ds(0, count)],
            dst_ref=part_recv.at[level, me_r, pl.ds(0, count)],
            send_sem=part_ssem.at[level, step],
            recv_sem=part_rsem.at[level, me_r],
            device_id=(me_d, aim(step)),
            device_id_type=MESH,
        )

    def await_part(level, rep, count):
        pltpu.make_async_remote_copy(
            src_ref=part_send.at[level, pl.ds(0, count)],
            dst_ref=part_recv.at[level, rep, pl.ds(0, count)],
            send_sem=part_ssem.at[level, 1],
            recv_sem=part_rsem.at[level, rep],
            device_id=(me_d, jnp.int32(rep)),
            device_id_type=MESH,
        ).wait_recv()

    def count_of(level, rep):
        return tile_rows if level and rep in ends else own_rows

    small = [
        pltpu.make_async_copy(hbm, ref, small_sem.at[i])
        for i, (hbm, ref) in enumerate(((rs_hbm, rs_ref), (dst_hbm, dst_ref), (src_hbm, src_ref)))
    ]
    for copy in small:
        copy.start()
    load_diag(0).start()
    for part in range(panels // chunk):
        load_panel(0, part).start()

    barrier = pltpu.get_barrier_semaphore()
    for j, step in everyone:
        pl.semaphore_signal(
            barrier,
            inc=1,
            device_id=(peer_dom(offsets[j]), peer_rep(step)),
            device_id_type=MESH,
        )

    def place(level):
        row = lax.broadcasted_iota(jnp.int32, (block, width), 0) // cols
        for t in range(tiles):
            twice = jnp.concatenate([rs_ref[level, t]] * (rep_size // 2), axis=0)
            placed[level, t * block : (t + 1) * block] = jnp.where(row == my_side, twice, 0.0)

    def share(level, partial):
        rounded = partial.astype(BF16)
        count = rounded.shape[0]
        part_send[level, :count] = rounded
        for step in others:
            send_part(level, step, count).start()
        part_recv[level, me_r, :count] = rounded

    def route():
        owner = me_d.astype(F32)
        row16 = iota((panels, panels), 0)
        col16 = iota((panels, panels), 1)
        lane = iota((1, 128), 1)
        id_level = div(lane, SLOTS)
        id_slot = lane - SLOTS * id_level
        panel_col = iota((panels, 1), 0)
        wanted = [jnp.zeros((1, 128), F32) for _ in range(HOOD)]
        for l in range(levels - 1):
            drow = dst_ref[l : l + 1, :].astype(F32)
            srow = src_ref[l : l + 1, :].astype(F32)
            dcol = jnp.sum(jnp.where(row16 == col16, drow, 0.0), axis=1, keepdims=True)
            scol = jnp.sum(jnp.where(row16 == col16, srow, 0.0), axis=1, keepdims=True)
            trow = jnp.where(drow >= 0, div(drow, tiles), -1.0)
            tcol = jnp.where(dcol >= 0, div(dcol, tiles), -1.0)
            earlier = (tcol == trow) & (drow >= 0) & (col16 < row16)
            rank = jnp.sum(jnp.where(earlier, 1.0, 0.0), axis=1, keepdims=True)
            away = tcol - owner
            away = away + jnp.where(away < 0, float(dom_size), 0.0)
            near = away + HALF
            near = near - jnp.where(near >= dom_size, float(dom_size), 0.0)
            reach = jnp.where(away == far, float(HOOD - 1), near)
            reach = jnp.where(dcol >= 0, reach, -1.0)
            spot = jnp.where(dcol >= 0, reach * SLOTS + rank, -1.0)
            tile = dcol - tiles * tcol
            here = spot == lane
            which = jnp.sum(jnp.where(here, panel_col, 0.0), axis=0, keepdims=True)
            source = jnp.sum(jnp.where(here, scol - zero_tile, 0.0), axis=0, keepdims=True)
            slots_v[2 * l : 2 * l + 1, :] = which.astype(jnp.int32)
            slots_v[2 * l + 1 : 2 * l + 2, :] = (source + zero_tile).astype(jnp.int32)
            mine = (rank == id_slot) & (id_level == l)
            for j in range(HOOD):
                found = jnp.where(mine & (reach == j), tile + 1.0, 0.0)
                wanted[j] = wanted[j] + jnp.sum(found, axis=0, keepdims=True)
        for j in range(HOOD):
            id_send[j] = (wanted[j] - 1.0).astype(jnp.int32)
        id_recv[HALF, me_r] = id_send[HALF]

    def learn_ids():
        for j, step in everyone:
            await_id(j, step)

        def lookup(ids, count, span, lane_in):
            lane_sender = div(iota((1, span), 1), span // count)
            take = jnp.where(iota((128, span), 0) == lane_in, 1.0, 0.0)
            every = jnp.dot(ids, take.astype(BF16), preferred_element_type=F32)
            own = jnp.where(iota((count, span), 0) == lane_sender, every, 0.0)
            return jnp.sum(own, axis=0, keepdims=True)

        near = jnp.zeros((pairs, 128), F32)
        full = jnp.zeros((senders, 128), F32)
        for j in range(HOOD):
            for turn in range(2):
                row = id_recv[j, 2 * my_side + turn].astype(F32)
                near = jnp.where(iota((pairs, 128), 0) == 2 * j + turn, row, near)
            for r in range(rep_size):
                row = id_recv[j, r].astype(F32)
                full = jnp.where(iota((senders, 128), 0) == rep_size * j + r, row, full)
        near, full = near.astype(BF16), full.astype(BF16)
        span = pairs * rows
        lane = iota((1, span), 1)
        lane_in = lane - rows * div(lane, rows)
        lane_slot = div(lane_in, block)
        lane_col = lane_in - block * lane_slot
        for l in range(last):
            tile = lookup(near, pairs, span, lane_slot + l * SLOTS)
            goal = jnp.where(tile >= 0, tile * block + lane_col, -1.0)
            unpack[l] = jnp.where(iota((tile_rows, span), 0) == goal, 1.0, 0.0).astype(BF16)
        span = senders * cols
        lane = iota((1, span), 1)
        lane_col = lane - cols * div(lane, cols)
        for l in range(levels - 1):
            for k in range(SLOTS):
                tile = lookup(full, senders, span, jnp.full((1, span), float(l * SLOTS + k), F32))
                goal = jnp.where(tile >= 0, tile * cols + lane_col, -1.0)
                unit_unpack[l, k] = jnp.where(iota((own_rows, span), 0) == goal, 1.0, 0.0).astype(BF16)

    def gather_units(level, arrived):
        residual = own_sides(level + 1)
        arrived = arrived.reshape(senders * cols, SLOTS * width)
        for k in range(SLOTS):
            residual = residual - jnp.dot(
                unit_unpack[level, k],
                arrived[:, k * width : (k + 1) * width],
                preferred_element_type=F32,
            )
        return residual

    def emit(level):
        for t in range(tiles):
            mine = solved_ref[level, t, my_half]
            picked = mine[:cols]
            for q in range(1, rep_size // 2):
                picked = jnp.where(my_side == q, mine[q * cols : (q + 1) * cols], picked)
            out_ref[level, t] = picked

    def own_sides(level):
        return jnp.concatenate([rs_ref[level, t] for t in range(tiles)], axis=0)

    small[0].wait()
    pl.semaphore_wait(barrier, len(everyone))
    share(0, own_sides(0))
    small[1].wait()
    small[2].wait()
    route()
    slot_copy = pltpu.make_async_copy(slots_v, slots_s, slot_sem)
    slot_copy.start()
    for j, step in everyone:
        send_id(j, step).start()
    for level in range(1, levels - 1):
        place(level)
    store[zero_tile] = jnp.zeros((2 * block, width), BF16)

    for level in range(levels - 1):
        for r in range(rep_size):
            pl.when(me_r != r)(lambda: await_part(level, r, count_of(level, r)))
        if level == 0:
            parts = [part_recv[0, r, :own_rows].astype(F32) for r in range(rep_size)]
            residuals = [
                jnp.concatenate(
                    [parts[r][t * cols : (t + 1) * cols] for r in ranking], axis=0
                )
                for t in range(tiles)
            ]
        else:
            total = part_recv[level, ends[0]].astype(F32) + part_recv[level, ends[1]].astype(F32)
            parts = [part_recv[level, r, :own_rows].astype(F32) for r in inner]
            residuals = [
                jnp.concatenate(
                    [total[t * block : (t + 1) * block]]
                    + [part[t * cols : (t + 1) * cols] for part in parts],
                    axis=0,
                )
                for t in range(tiles)
            ]
        load_diag(level).wait()
        for t in range(tiles):
            residual = residuals[t].astype(BF16)
            solved = jnp.dot(residual, diag[level, t], preferred_element_type=F32)
            store[level * tiles + t] = solved.astype(BF16)
            for h in range(2):
                solved_ref[level, t, h] = solved[h * block : (h + 1) * block]
        if level == 0:
            slot_copy.wait()
        for part in range(panels // chunk):
            load_panel(level, part).wait()
        for group in val_groups if level < last else last_groups:
            products = {}
            for j in group:
                for k in range(SLOTS):
                    which = jnp.clip(slots_s[2 * level, j * SLOTS + k], 0, panels - 1)
                    source = jnp.clip(slots_s[2 * level + 1, j * SLOTS + k], 0, zero_tile)
                    products[j, k] = jnp.dot(
                        store[source], panels_by_level[level][which], preferred_element_type=F32
                    )
            for j in group:
                if level < last:
                    for k in range(SLOTS):
                        rounded = products[j, k].astype(BF16)
                        val_send[level, j, k * block : (k + 1) * block] = rounded[:block]
                        for m in range(2):
                            begin = block + m * cols
                            unit_send[level, j, m, :, k * width : (k + 1) * width] = products[j, k][
                                begin : begin + cols
                            ].astype(BF16)
                else:
                    for r in range(rep_size):
                        begin = ranking.index(r) * cols
                        piece = [products[j, k][begin : begin + cols] for k in range(SLOTS)]
                        for k in range(SLOTS):
                            last_send[j, r, :, k * width : (k + 1) * width] = piece[k].astype(BF16)
            if level < last:
                each_val(level, group, lambda copy: copy.start())
            else:
                for step in others + [0]:
                    for j in group:
                        if (j, step) in everyone:
                            send_last(j, step).start()
        if level < last:

            @pl.when(is_end)
            def _():
                val_recv[level, HALF, my_turn] = val_send[level, HALF]

            @pl.when(is_inner)
            def _():
                unit_recv[level, HALF, me_r] = unit_send[level, HALF, my_unit]

        else:
            last_recv[HALF, me_r] = last_send[HALF, me_r]
        load_diag(level + 1).start()
        if level < last:
            for part in range(panels // chunk):
                load_panel(level + 1, part).start()
        if level == 0:
            learn_ids()
        emit(level)
        if level < last:

            @pl.when(is_end)
            def _():
                for j in order:
                    for other in (True, False):
                        if other or offsets[j] != 0:
                            await_val(level, j, other)
                arrived = val_recv[level].reshape(pairs * rows, width)
                incoming = jnp.dot(unpack[level], arrived, preferred_element_type=F32)
                share(level + 1, placed[level + 1] - incoming)

            @pl.when(is_inner)
            def _():
                for j, step in everyone:
                    await_unit(level, j, step)
                share(level + 1, gather_units(level, unit_recv[level]))

    for j, step in everyone:
        await_last(j, step)
    residual = gather_units(last, last_recv[...])
    residual = residual.astype(BF16)
    load_diag(levels - 1).wait()
    for t in range(tiles):
        solved = jnp.dot(residual, diag[levels - 1, t], preferred_element_type=F32)
        out_ref[levels - 1, t] = solved[t * cols : (t + 1) * cols]

    for j, step in everyone:
        send_id(j, step).wait_send()
        send_last(j, step).wait_send()
    for level in range(last):
        each_val(level, order, lambda copy: copy.wait_send())
    for step in others:
        send_part(0, step, own_rows).wait_send()
        for level in range(1, levels - 1):
            pl.when(is_end)(lambda: send_part(level, step, tile_rows).wait_send())
            pl.when(is_inner)(lambda: send_part(level, step, own_rows).wait_send())


def per_device(right_sides, diag_inverse, panel_mats, panel_src, panel_dst):
    levels, tiles, cols, width = right_sides.shape
    panels = panel_mats.shape[1]
    dom_size = lax.axis_size("dom")
    rep_size = lax.axis_size("rep")
    block = rep_size // 2 * cols
    tile_rows = tiles * block
    rows = SLOTS * block
    chunk = 4 if panels % 4 == 0 else 1
    assert rep_size == 4 and block % 8 == 0 and (levels - 1) * SLOTS <= 128 and levels > 2
    dims = (levels, tiles, cols, width, panels, dom_size, rep_size, chunk)
    vmem = pl.BlockSpec(memory_space=pltpu.VMEM)
    hbm = pl.BlockSpec(memory_space=pl.ANY)
    dma = pltpu.SemaphoreType.DMA
    i32 = jnp.int32
    return pl.pallas_call(
        functools.partial(kernel, dims),
        out_shape=jax.ShapeDtypeStruct(right_sides.shape, F32),
        in_specs=[hbm] * 5,
        out_specs=vmem,
        scratch_shapes=[
            pltpu.VMEM(panel_src.shape, i32),
            pltpu.VMEM(panel_dst.shape, i32),
            pltpu.VMEM(right_sides.shape, F32),
            dma((3,)),
            pltpu.VMEM(diag_inverse.shape, BF16),
            [pltpu.VMEM(panel_mats.shape[1:], BF16) for _ in range(levels - 1)],
            pltpu.VMEM(((levels - 1) * tiles + 1, 2 * block, width), BF16),
            pltpu.VMEM((levels - 1, tiles, 2, block, width), F32),
            pltpu.VMEM((levels - 1, tile_rows, width), F32),
            pltpu.VMEM((8, 128), i32),
            pltpu.SMEM((8, 128), i32),
            dma,
            pltpu.VMEM((levels - 2, HOOD, rows, width), BF16),
            pltpu.VMEM((levels - 2, HOOD, 2, rows, width), BF16),
            pltpu.VMEM((levels - 2, tile_rows, 2 * HOOD * rows), BF16),
            pltpu.VMEM((levels - 1, tile_rows, width), BF16),
            pltpu.VMEM((levels - 1, rep_size, tile_rows, width), BF16),
            pltpu.VMEM((HOOD, 1, 128), i32),
            pltpu.VMEM((HOOD, rep_size, 1, 128), i32),
            pltpu.VMEM((levels - 2, HOOD, 2, cols, SLOTS * width), BF16),
            pltpu.VMEM((levels - 2, HOOD, rep_size, cols, SLOTS * width), BF16),
            pltpu.VMEM((levels - 1, SLOTS, tiles * cols, HOOD * rep_size * cols), BF16),
            pltpu.VMEM((HOOD, rep_size, cols, SLOTS * width), BF16),
            pltpu.VMEM((HOOD, rep_size, cols, SLOTS * width), BF16),
            dma((levels,)),
            dma((levels - 1, panels // chunk)),
            dma((levels - 2, HOOD)),
            dma((levels - 2, HOOD, 2)),
            dma((levels - 1, rep_size)),
            dma((levels - 1, rep_size)),
            dma((HOOD, rep_size)),
            dma((HOOD, rep_size)),
            dma((levels - 2, HOOD, 2)),
            dma((levels - 2, HOOD, rep_size)),
            dma((HOOD, rep_size)),
            dma((HOOD, rep_size)),
        ],
        compiler_params=pltpu.CompilerParams(
            collective_id=0, has_side_effects=True, vmem_limit_bytes=67043328
        ),
    )(panel_src, panel_dst, right_sides, diag_inverse, panel_mats)


def solution(mesh):
    return jax.shard_map(
        per_device,
        mesh=mesh,
        in_specs=(
            P(None, "dom", "rep", None),
            P(None, "dom", None, None),
            P(None, ("dom", "rep"), None, None),
            P(None, ("dom", "rep")),
            P(None, ("dom", "rep")),
        ),
        out_specs=P(None, "dom", "rep", None),
        check_vma=False,
    )
```
